32 devices in a mesh: dom: 32 (over z, y, x, core).
Axes of the slice: x: 2, y: 2, z: 4, core: 2. Of those that a mesh axis runs over, the one named last changes fastest.
Arguments:
- features: bfloat16 [32768, 256], P('dom'), may hold values from -6 to 6
- edge_source: int32 [32, 128, 128], P('dom'), may hold values from 0 to 2047, as said below
- edge_relation: int32 [32, 128, 128], P('dom'), may hold values from 0 to 7
- edge_target: int32 [32, 128, 128], P('dom'), may hold values from 0 to 1023, as said below
- block_count: int32 [32], P('dom'), may hold values from 1 to 128, as said below
- send_list: int32 [32, 32, 32], P('dom'), may hold values from 0 to 1023
- bases_first: bfloat16 [30, 256, 256], P(None, 'dom'), may hold values from -0.375 to 0.375
- self_first: bfloat16 [256, 256], P('dom'), may hold values from -0.375 to 0.375
- coef_first: float32 [8, 30], replicated, may hold values from -1 to 1
- bias_first: float32 [256], replicated, may hold values from -3 to 3
- bases_second: bfloat16 [30, 256, 256], P(None, 'dom'), may hold values from -0.375 to 0.375
- self_second: bfloat16 [256, 256], P('dom'), may hold values from -0.375 to 0.375
- coef_second: float32 [8, 30], replicated, may hold values from -1 to 1
- bias_second: float32 [256], replicated, may hold values from -3 to 3
Outputs:
- embedded: bfloat16 [32768, 256], P('dom')
The draws below stay inside these ranges and needn't reach their ends.
Inputs may be any that keep to these rules, and one draw needn't show every extreme that they name: `edge_source`: an entry below 1024 names a row of the edge's own partition; an entry 1024 + p * 32 + s names the row that partition p sends to the edge's partition in slot s, and p is never the edge's own partition. `edge_target`: non-decreasing within each block; all targets of one block lie in one aligned window of 16 rows, from 16 * k to 16 * k + 15 for some k. `block_count`: blocks at and beyond it are ignored; some partition uses all 128.
All inputs are finite; a program needn't handle non-finite values.
Results may differ from the reference program's by a relative error of at most 0.0064.
Values may be sent and summed in bfloat16 or wider, within the bound.
A program may use at most 128 MiB of HBM per device.

```python
import jax
import jax.numpy as jnp
from jax import lax

D = 256
REL = 8
BASES = 30
NODE_DEV = 1024
SLOT = 32
BLOCKS = 128
EBLK = 128
WIN = 16
NODES = 32768
N_DOM = 32


def draw_edge_source(key, part):
    key_used, key_local, key_offset, key_slot, key_remote = jax.random.split(key, 5)
    shape = (N_DOM, BLOCKS, EBLK)
    sent_counts = jax.random.randint(key_used, (N_DOM, N_DOM), SLOT // 4, SLOT + 1)
    local_rows = jax.random.randint(key_local, shape, 0, NODE_DEV)
    offset = jax.random.randint(key_offset, shape, 1, N_DOM)
    target_part = jnp.arange(N_DOM, dtype=jnp.int32)[:, None, None]
    owner = (target_part + offset) % N_DOM
    limit = sent_counts[owner, target_part]
    slot_index = jax.random.randint(key_slot, shape, 0, 1 << 20) % limit
    remote = jax.random.randint(key_remote, shape, 0, 2) == 1
    return jnp.where(remote, NODE_DEV + owner * SLOT + slot_index, local_rows).astype(jnp.int32)


def draw_edge_target(key, part):
    key_window, key_offset = jax.random.split(key)
    windows = jnp.sort(jax.random.randint(key_window, (N_DOM, BLOCKS), 0, NODE_DEV // WIN), axis=1)
    offsets = jnp.sort(jax.random.randint(key_offset, (N_DOM, BLOCKS, EBLK), 0, WIN), axis=2)
    return (windows[:, :, None] * WIN + offsets).astype(jnp.int32)


def draw_block_count(key, part):
    key_counts, key_top = jax.random.split(key)
    counts = jax.random.randint(key_counts, (N_DOM,), max(BLOCKS // 2, 1), BLOCKS + 1)
    busiest = jax.random.randint(key_top, (), 0, N_DOM)
    return counts.at[busiest].set(BLOCKS).astype(jnp.int32)


def place_ends(entries, own_key, least, largest):
    spot = [jax.random.randint(jax.random.fold_in(own_key, axis), (), 0, length) for axis, length in enumerate(entries.shape)]
    main_axis = entries.shape.index(max(entries.shape))
    next_to = spot[:main_axis] + [(spot[main_axis] + 1) % entries.shape[main_axis]] + spot[main_axis + 1:]
    return entries.at[tuple(spot)].set(least).at[tuple(next_to)].set(largest)


def steps_of(own_key, shape, cuts, least, top_value):
    loudness = 1.0
    for dim, blocks in cuts:
        heights = jax.random.uniform(jax.random.fold_in(jax.random.fold_in(own_key, 6), dim), (blocks,), jnp.float32, least / len(cuts), top_value / len(cuts))
        loudness = loudness * jnp.repeat(jnp.exp(heights), shape[dim] // blocks).reshape((-1,) + (1,) * (len(shape) - 1 - dim))
    return loudness


def scatter_about(rng, dims, deviation, most, pieces=(), kind=jnp.bfloat16):
    drawn = deviation * jax.random.normal(rng, dims, jnp.float32)
    if pieces:
        drawn = drawn * steps_of(rng, dims, pieces, -0.22, 0.18)
    return jnp.clip(drawn, -most, most).astype(kind)


def setup_inputs(seed: int = 0) -> dict:
    streams_of = jax.random.split(jax.random.key(seed), 15)
    return {
        "features": scatter_about(streams_of[0], (NODES, D), 1.0, 6.0, ((0, 32),)),
        "edge_source": draw_edge_source(jax.random.fold_in(streams_of[14], 71), 0),
        "edge_relation": place_ends(jax.random.randint(streams_of[2], (N_DOM, BLOCKS, EBLK), 0, REL), jax.random.fold_in(streams_of[2], 1), 0, REL - 1).astype(jnp.int32),
        "edge_target": draw_edge_target(jax.random.fold_in(streams_of[14], 71), 0),
        "block_count": draw_block_count(jax.random.fold_in(streams_of[14], 71), 0),
        "send_list": place_ends(jax.random.randint(streams_of[5], (N_DOM, N_DOM, SLOT), 0, NODE_DEV), jax.random.fold_in(streams_of[5], 1), 0, NODE_DEV - 1).astype(jnp.int32),
        "bases_first": scatter_about(streams_of[6], (BASES, D, D), D ** -0.5, 0.375, ((1, 32),)),
        "self_first": scatter_about(streams_of[7], (D, D), D ** -0.5, 0.375, ((0, 32),)),
        "coef_first": scatter_about(streams_of[8], (REL, BASES), BASES ** -0.5, 1.0, (), jnp.float32),
        "bias_first": scatter_about(streams_of[9], (D,), 0.5, 3.0, (), jnp.float32),
        "bases_second": scatter_about(streams_of[10], (BASES, D, D), D ** -0.5, 0.375, ((1, 32),)),
        "self_second": scatter_about(streams_of[11], (D, D), D ** -0.5, 0.375, ((0, 32),)),
        "coef_second": scatter_about(streams_of[12], (REL, BASES), BASES ** -0.5, 1.0, (), jnp.float32),
        "bias_second": scatter_about(streams_of[13], (D,), 0.5, 3.0, (), jnp.float32),
    }


def compose_weights(coef, bases):
    mixed = jnp.einsum("rb,bij->rij", coef, bases.astype(jnp.float32), precision=lax.Precision.HIGHEST)
    return mixed.astype(jnp.bfloat16)


def relational_layer(inputs_now, edge_source, edge_relation, edge_target, block_count, send_list, mixed, self_weight, bias):
    owners = jnp.arange(N_DOM, dtype=jnp.int32)

    def one_part(part_index):
        received = inputs_now[owners[:, None], send_list[:, part_index, :]].reshape(-1, D)
        row_table = jnp.concatenate([inputs_now[part_index], received], axis=0)
        sources = edge_source[part_index].reshape(-1)
        relation_ids = edge_relation[part_index].reshape(-1)
        targets = edge_target[part_index].reshape(-1)
        block_ids = lax.broadcasted_iota(jnp.int32, (BLOCKS, EBLK), 0).reshape(-1)
        in_use = block_ids < block_count[part_index]
        messages = row_table[sources].astype(jnp.float32)
        segment = jnp.where(in_use, targets * REL + relation_ids, NODE_DEV * REL)
        degree = jax.ops.segment_sum(jnp.ones(segment.shape, jnp.float32), segment, NODE_DEV * REL + 1)[:NODE_DEV * REL]
        pooled = jax.ops.segment_sum(messages, segment, NODE_DEV * REL + 1)[:NODE_DEV * REL]
        averaged = (pooled / jnp.maximum(degree, 1.0)[:, None]).astype(jnp.bfloat16).reshape(NODE_DEV, REL, D)
        summed_all = jnp.dot(inputs_now[part_index], self_weight, preferred_element_type=jnp.float32) + bias
        for relation in range(REL):
            summed_all = summed_all + jnp.dot(averaged[:, relation, :], mixed[relation], preferred_element_type=jnp.float32)
        return summed_all

    return lax.map(one_part, owners)


def reference(features, edge_source, edge_relation, edge_target, block_count, send_list, bases_first, self_first, coef_first, bias_first, bases_second, self_second, coef_second, bias_second):
    inputs_now = features.reshape(N_DOM, NODE_DEV, D)
    mixed_first = compose_weights(coef_first, bases_first)
    first = relational_layer(inputs_now, edge_source, edge_relation, edge_target, block_count, send_list, mixed_first, self_first, bias_first)
    hidden = jnp.maximum(first, 0.0).astype(jnp.bfloat16)
    mixed_second = compose_weights(coef_second, bases_second)
    second = relational_layer(hidden, edge_source, edge_relation, edge_target, block_count, send_list, mixed_second, self_second, bias_second)
    return second.astype(jnp.bfloat16).reshape(N_DOM * NODE_DEV, D)
```

```python
import functools
import math

import jax
import jax.numpy as jnp
from jax import lax
from jax.experimental import pallas as pl
from jax.experimental.pallas import tpu as pltpu
from jax.sharding import PartitionSpec as P

WIN = 16
OWN, NEAR, FAR, COUNT, SPREAD = 16, 16, 16, 32, 16
VMEM_LIMIT = 63 * 1024 * 1024
MESH = pl.DeviceIdType.MESH


def sides(devices):
    chips = devices // 2
    side = max(math.isqrt(chips // 4), 1)
    return chips // (side * side), side, side, 2


def one_hot(columns, first, count):
    lanes = lax.broadcasted_iota(jnp.int32, columns.shape, 1)
    parts = [
        (columns == lanes + (first + part * 128)).astype(jnp.float32).astype(jnp.bfloat16)
        for part in range(count // 128)
    ]
    return jnp.concatenate(parts, axis=1)


def fused_kernel(
    devices,
    source_ref,
    relation_ref,
    target_ref,
    send_ref,
    count_ref,
    features_ref,
    bases_a,
    self_a,
    bases_b,
    self_b,
    coef_a,
    coef_b,
    bias_a,
    bias_b,
    out_ref,
    column_ref,
    picked_ref,
    pooled_ref,
    inverse_ref,
    mean_ref,
    weight_ref,
    pieces_a,
    pieces_b,
    slot_ref,
    send_column_ref,
    sent,
    came_a,
    came_b,
    hidden_ref,
    plan_ref,
    plan_smem,
    plan_sem,
    send_sems,
    recv_sems,
    piece_send_sems,
    piece_recv_sems,
):
    me = lax.axis_index("dom")
    planes, rows_y, rows_x, cores = sides(devices)
    low = rows_y * rows_x * cores
    my_z, my_low = me // low, me % low
    my_y = my_low // (rows_x * cores)
    my_x = my_low // cores % rows_x
    my_core = my_low % cores
    node_rows, width = features_ref.shape
    blocks, edges = source_ref.shape
    peers, slots = send_ref.shape
    relations, bases = coef_a.shape
    share = self_a.shape[0]
    windows = node_rows // WIN
    places = WIN * relations
    plane_rows = low * slots

    def at(z, y, x, core):
        return ((z * rows_y + y) * rows_x + x) * cores + core

    barrier = pltpu.get_barrier_semaphore()

    def greet(hop, carry):
        peer = lax.rem(me + hop, devices)
        pl.semaphore_signal(barrier, inc=1, device_id=(peer,), device_id_type=MESH)
        return carry

    lax.fori_loop(1, devices, greet, 0)

    def compose(bases_ref, self_ref, coef_ref, pieces):
        sums = [jnp.zeros((share, width), jnp.float32) for _ in range(relations)]
        for basis in range(bases):
            matrix = bases_ref[basis].astype(jnp.float32)
            sums = [
                total + coef_ref[relation, basis] * matrix for relation, total in enumerate(sums)
            ]
        for relation, total in enumerate(sums):
            pieces[my_z, my_y, my_x, my_core, relation] = total.astype(jnp.bfloat16)
        pieces[my_z, my_y, my_x, my_core, relations] = self_ref[...]

    compose(bases_a, self_a, coef_a, pieces_a)
    compose(bases_b, self_b, coef_b, pieces_b)

    lane_ids = lax.broadcasted_iota(jnp.int32, (edges, 128), 1)
    row_ids = lax.broadcasted_iota(jnp.int32, (edges, 128), 0)
    eye = row_ids == lane_ids
    eye_send = lax.broadcasted_iota(jnp.int32, (slots, slots), 0) == lax.broadcasted_iota(
        jnp.int32, (slots, slots), 1
    )

    def send_columns(group, carry):
        listed = send_ref[pl.ds(pl.multiple_of(group * 8, 8), 8), :]
        for row in range(8):
            spread = jnp.where(eye_send, listed[row : row + 1, :], 0).astype(jnp.float32)
            column = jnp.sum(spread, axis=1, keepdims=True)
            first = pl.multiple_of((group * 8 + row) * slots, slots)
            send_column_ref[pl.ds(first, slots), :] = jnp.broadcast_to(
                column, (slots, 128)
            ).astype(jnp.int32)
        return carry

    lax.fori_loop(0, peers // 8, send_columns, 0)

    def plan():
        window_c = jnp.broadcast_to(target_ref[:, 0:1] // WIN, (blocks, 128))
        window_r = jnp.sum(jnp.where(eye, window_c, 0), axis=0, keepdims=True)
        key_c = window_c * blocks + row_ids
        key_r = window_r * blocks + lane_ids[0:1]
        before = jnp.where(key_c < key_r, 1, 0)
        rank_r = jnp.sum(before, axis=0, keepdims=True)
        same = jnp.where(window_c == window_r, before, 0)
        follows_r = jnp.minimum(jnp.sum(same, axis=0, keepdims=True), 1)
        rank_c = jnp.transpose(jnp.broadcast_to(rank_r, (128, 128)))
        follows_c = jnp.transpose(jnp.broadcast_to(follows_r, (128, 128)))
        placed = rank_c == lane_ids
        order = jnp.sum(jnp.where(placed, row_ids, 0), axis=0, keepdims=True)
        keep = jnp.sum(jnp.where(placed, follows_c, 0), axis=0, keepdims=True)
        last = jnp.max(
            jnp.where(window_c == lane_ids, rank_c + 1, 0), axis=0, keepdims=True
        )
        plan_ref[...] = jnp.concatenate(
            [order, keep, last, jnp.zeros((5, 128), jnp.int32)], axis=0
        )

    plan()

    slot = relation_ref[...] * WIN + target_ref[...] % WIN
    slot_ref[...] = jnp.where(row_ids < count_ref[0], slot, -1).reshape(blocks, 1, edges)

    def copies(layer, stage):
        pieces = (pieces_a, pieces_b)[layer]
        made = []
        if stage == 0:
            count, source = planes, lambda: pieces.at[my_z, my_y, my_x, my_core]
        elif stage == 1:
            count, source = rows_y, lambda: pieces.at[:, my_y, my_x, my_core]
        elif stage == 2:
            count, source = rows_x, lambda: pieces.at[:, :, my_x, my_core]
        else:
            count, source = cores, lambda: pieces.at[:, :, :, my_core]
        for hop in range(1, count):
            to = [my_z, my_y, my_x, my_core]
            to[stage] = lax.rem(to[stage] + hop, count)
            by = [my_z, my_y, my_x, my_core]
            by[stage] = lax.rem(by[stage] + count - hop, count)
            landed = pieces.at[(*(slice(None),) * stage, by[stage], *by[stage + 1 :])]
            if stage == 0:
                landed = pieces.at[by[0], my_y, my_x, my_core]
            pair = (layer, stage, hop)
            sems = dict(
                send_sem=piece_send_sems.at[pair],
                recv_sem=piece_recv_sems.at[pair],
                device_id=(at(*to),),
                device_id_type=MESH,
            )
            made.append(
                (
                    pltpu.make_async_remote_copy(src_ref=source(), dst_ref=source(), **sems),
                    pltpu.make_async_remote_copy(src_ref=landed, dst_ref=landed, **sems),
                )
            )
        return made

    def send_pieces(layer, stage):
        for out, _ in copies(layer, stage):
            out.start()

    def land_pieces(layer, stage):
        for out, landed in copies(layer, stage):
            out.wait_send()
            landed.wait_recv()

    def join_pieces(layer):
        pieces = (pieces_a, pieces_b)[layer]

        group = max(16 // share, 1)
        height = group * share

        def join(step, carry):
            for relation in range(relations + 1):
                rows = []
                for part in range(group):
                    device = step * group + part
                    z, rest = device // low, device % low
                    y, rest = rest // (rows_x * cores), rest % (rows_x * cores)
                    rows.append(
                        pieces[z, y, rest // cores, rest % cores, relation].astype(jnp.float32)
                    )
                first = pl.multiple_of(step * height, height)
                weight_ref[relation, pl.ds(first, height), :] = (
                    rows[0] if group == 1 else jnp.concatenate(rows, axis=0)
                ).astype(jnp.bfloat16)
            return carry

        lax.fori_loop(0, devices // group, join, 0)

    def peer_of(hop_z, hop_low, sign):
        z = lax.rem(my_z + planes + sign * hop_z, planes)
        rest = lax.rem(my_low + low + sign * hop_low, low)
        return z * low + rest

    def row_copy(layer, hop_z, hop_low, landing):
        came = (came_a, came_b)[layer]
        hop = hop_z * low + hop_low
        to = peer_of(hop_z, hop_low, 1)
        owner = peer_of(hop_z, hop_low, -1) if landing else me
        return pltpu.make_async_remote_copy(
            src_ref=sent.at[pl.ds(pl.multiple_of(to * slots, slots), slots)],
            dst_ref=came.at[pl.ds(pl.multiple_of(owner * slots, slots), slots)],
            send_sem=send_sems.at[layer, hop],
            recv_sem=recv_sems.at[layer, hop],
            device_id=(to,),
            device_id_type=MESH,
        )

    def plane_order():
        return sorted(range(planes), key=lambda hop: -min(hop, planes - hop))

    def pick_plane(layer, rows_ref, hop_z):
        z = lax.rem(my_z + hop_z, planes)
        for part in range(plane_rows // 256):
            first = pl.multiple_of(z * plane_rows + part * 256, 256)
            hot = one_hot(send_column_ref[pl.ds(first, 256), :], 0, node_rows)
            sent[pl.ds(first, 256), :] = jnp.dot(
                hot, rows_ref[...], preferred_element_type=jnp.float32
            ).astype(jnp.bfloat16)

    def start_plane(layer, hop_z):
        def start(hop_low, carry):
            row_copy(layer, hop_z, hop_low, False).start()
            return carry

        lax.fori_loop(1 if hop_z == 0 else 0, low, start, 0)

    def land_plane(layer, hop_z):
        def land(hop_low, carry):
            row_copy(layer, hop_z, hop_low, False).wait_send()
            row_copy(layer, hop_z, hop_low, True).wait_recv()
            return carry

        lax.fori_loop(1 if hop_z == 0 else 0, low, land, 0)

    place_ids = lax.broadcasted_iota(jnp.int32, (places, edges), 0)

    def send_rows(layer, rows_ref):
        came = (came_a, came_b)[layer]
        came[pl.ds(pl.multiple_of(me * slots, slots), slots), :] = jnp.zeros(
            (slots, width), jnp.bfloat16
        )
        waiting = None
        for hop_z in plane_order():
            pick_plane(layer, rows_ref, hop_z)
            if waiting is not None:
                start_plane(layer, waiting)
            waiting = hop_z
        return waiting

    def own_stage(rows_ref):
        def pick(step, carry):
            part = pl.ds(step * OWN, OWN)
            hot = one_hot(column_ref[part].reshape(OWN * edges, 128), 0, node_rows)
            picked_ref[part] = (
                jnp.dot(hot, rows_ref[...], preferred_element_type=jnp.float32)
                .astype(jnp.bfloat16)
                .reshape(OWN, edges, width)
            )
            return carry

        lax.fori_loop(0, blocks // OWN, pick, 0)

    def plane_parts(layer, columns, hops):
        came = (came_a, came_b)[layer]
        total = None
        for hop_z in hops:
            z = lax.rem(my_z + planes - hop_z, planes)
            hot = one_hot(columns, node_rows + z * plane_rows, plane_rows)
            rows = came[pl.ds(pl.multiple_of(z * plane_rows, plane_rows), plane_rows), :]
            part = jnp.dot(hot, rows, preferred_element_type=jnp.float32)
            total = part if total is None else total + part
        return total.astype(jnp.bfloat16)

    def near_stage(layer, hops):
        def pick(step, carry):
            part = pl.ds(step * NEAR, NEAR)
            columns = column_ref[part].reshape(NEAR * edges, 128)
            picked_ref[part] += plane_parts(layer, columns, hops).reshape(NEAR, edges, width)
            return carry

        lax.fori_loop(0, blocks // NEAR, pick, 0)

    def block_at(step):
        return jnp.clip(plan_smem[0, step], 0, blocks - 1)

    def last_of(window):
        return jnp.clip(plan_smem[2, window], 0, blocks)

    def hot_of(block):
        return (place_ids == slot_ref[block]).astype(jnp.float32).astype(jnp.bfloat16)

    def far_stage(layer, hops):
        def pool(step, carry):
            named = [block_at(step * FAR + part) for part in range(FAR)]
            columns = jnp.concatenate([column_ref[block] for block in named], axis=0)
            gathered = plane_parts(layer, columns, hops)
            total = pooled_ref[step * FAR]
            for part in range(FAR):
                messages = (
                    gathered[part * edges : (part + 1) * edges] + picked_ref[named[part]]
                )
                sums = jnp.dot(
                    hot_of(named[part]), messages, preferred_element_type=jnp.float32
                )
                keep = plan_smem[1, step * FAR + part].astype(jnp.float32)
                total = total * keep + sums
                pooled_ref[step * FAR + part + 1] = total
            return carry

        lax.fori_loop(0, blocks // FAR, pool, 0)

    def degree_stage():
        ones = jnp.ones((edges, 128), jnp.bfloat16)

        def pool(step, carry):
            total = pooled_ref[step * COUNT, :, 0:128]
            for part in range(COUNT):
                block = block_at(step * COUNT + part)
                numbers = jnp.dot(hot_of(block), ones, preferred_element_type=jnp.float32)
                keep = plan_smem[1, step * COUNT + part].astype(jnp.float32)
                total = total * keep + numbers
                pooled_ref[step * COUNT + part + 1, :, 0:128] = total
            return carry

        lax.fori_loop(0, blocks // COUNT, pool, 0)

        def invert(window, carry):
            numbers = pooled_ref[last_of(window), :, 0:128]
            inverse_ref[window] = 1.0 / jnp.maximum(numbers, 1.0)
            return carry

        lax.fori_loop(0, windows, invert, 0)

    def mean_stage():
        def average(window, carry):
            block = last_of(window)
            first = pl.multiple_of(window * WIN, WIN)
            for relation in range(relations):
                part = slice(relation * WIN, (relation + 1) * WIN)
                inverse = inverse_ref[window, part, :]
                for lane in range(0, width, 128):
                    mean_ref[relation, pl.ds(first, WIN), lane : lane + 128] = (
                        pooled_ref[block, part, lane : lane + 128] * inverse
                    ).astype(jnp.bfloat16)
            return carry

        lax.fori_loop(0, windows, average, 0)

    def dense_stage(rows_ref, bias_ref, result_ref, last):
        def dense(chunk, carry):
            rows = pl.ds(pl.multiple_of(chunk * 256, 256), 256)
            total = bias_ref[...] + jnp.dot(
                rows_ref[rows, :], weight_ref[relations], preferred_element_type=jnp.float32
            )
            for relation in range(relations):
                total = total + jnp.dot(
                    mean_ref[relation, rows, :],
                    weight_ref[relation],
                    preferred_element_type=jnp.float32,
                )
            if not last:
                total = jnp.maximum(total, 0.0)
            result_ref[rows, :] = total.astype(jnp.bfloat16)
            return carry

        lax.fori_loop(0, node_rows // 256, dense, 0)

    def source_columns():
        turned = jnp.transpose(source_ref[...].astype(jnp.float32))

        def spread(group, carry):
            rolled = pltpu.roll(turned, blocks - group * SPREAD, 1)
            for row in range(SPREAD):
                column_ref[group * SPREAD + row] = jnp.broadcast_to(
                    rolled[:, row : row + 1], (edges, 128)
                ).astype(jnp.int32)
            return carry

        lax.fori_loop(0, blocks // SPREAD, spread, 0)

    near = [planes // 2, 0] if planes > 2 else list(range(planes))
    far = [hop for hop in range(planes) if hop not in near]

    scope = jax.named_scope
    plan_copy = pltpu.make_async_copy(plan_ref, plan_smem, plan_sem)
    with scope("columns"):
        source_columns()
    plan_copy.start()
    pooled_ref[0] = jnp.zeros(pooled_ref.shape[1:], jnp.float32)
    with scope("greeted"):
        pl.semaphore_wait(barrier, devices - 1)
    send_pieces(0, 0)
    with scope("send_a"):
        waiting = send_rows(0, features_ref)
    plan_copy.wait()
    start_plane(0, waiting)
    with scope("degree"):
        degree_stage()
    with scope("piece_z"):
        land_pieces(0, 0)
    send_pieces(0, 1)
    with scope("own_a"):
        own_stage(features_ref)
    with scope("piece_y"):
        land_pieces(0, 1)
    send_pieces(0, 2)
    with scope("land_near_a"):
        for hop in near:
            land_plane(0, hop)
    with scope("near_a"):
        near_stage(0, near)
    with scope("land_far_a"):
        for hop in far:
            land_plane(0, hop)
    with scope("piece_x"):
        land_pieces(0, 2)
    send_pieces(0, 3)
    send_pieces(1, 0)
    with scope("far_a"):
        far_stage(0, far)
    with scope("piece_z_b"):
        land_pieces(1, 0)
    send_pieces(1, 1)
    with scope("mean_a"):
        mean_stage()
    with scope("piece_core"):
        land_pieces(0, 3)
    with scope("join_a"):
        join_pieces(0)
    with scope("dense_a"):
        dense_stage(features_ref, bias_a, hidden_ref, False)

    with scope("piece_y_b"):
        land_pieces(1, 1)
    send_pieces(1, 2)
    with scope("send_b"):
        waiting = send_rows(1, hidden_ref)
    start_plane(1, waiting)
    with scope("own_b"):
        own_stage(hidden_ref)
    with scope("piece_x_b"):
        land_pieces(1, 2)
    send_pieces(1, 3)
    with scope("land_near_b"):
        for hop in near:
            land_plane(1, hop)
    with scope("near_b"):
        near_stage(1, near)
    with scope("piece_core_b"):
        land_pieces(1, 3)
    with scope("join_b"):
        join_pieces(1)
    with scope("land_far_b"):
        for hop in far:
            land_plane(1, hop)
    with scope("far_b"):
        far_stage(1, far)
    with scope("mean_b"):
        mean_stage()
    with scope("dense_b"):
        dense_stage(hidden_ref, bias_b, out_ref, True)


def in_smem():
    return pl.BlockSpec(memory_space=pltpu.SMEM)


def in_vmem():
    return pl.BlockSpec(memory_space=pltpu.VMEM)


def shards(
    devices,
    features,
    edge_source,
    edge_relation,
    edge_target,
    block_count,
    send_list,
    bases_first,
    self_first,
    coef_first,
    bias_first,
    bases_second,
    self_second,
    coef_second,
    bias_second,
):
    node_rows, width = features.shape
    _, blocks, edges = edge_source.shape
    _, peers, slots = send_list.shape
    relations = coef_first.shape[0]
    share = self_first.shape[0]
    planes, rows_y, rows_x, cores = sides(devices)
    windows = node_rows // WIN
    places = WIN * relations
    came = peers * slots
    bf16, f32, i32 = jnp.bfloat16, jnp.float32, jnp.int32
    piece = (planes, rows_y, rows_x, cores, relations + 1, share, width)
    most = max(planes, rows_y, rows_x, cores)
    return pl.pallas_call(
        functools.partial(fused_kernel, devices),
        out_shape=jax.ShapeDtypeStruct((node_rows, width), bf16),
        in_specs=[in_vmem()] * 4
        + [in_smem()]
        + [in_vmem()] * 5
        + [in_smem()] * 2
        + [in_vmem()] * 2,
        out_specs=in_vmem(),
        scratch_shapes=[
            pltpu.VMEM((blocks, edges, 128), i32),
            pltpu.VMEM((blocks, edges, width), bf16),
            pltpu.VMEM((blocks + 1, places, width), f32),
            pltpu.VMEM((windows, places, 128), f32),
            pltpu.VMEM((relations, node_rows, width), bf16),
            pltpu.VMEM((relations + 1, width, width), bf16),
            pltpu.VMEM(piece, bf16),
            pltpu.VMEM(piece, bf16),
            pltpu.VMEM((blocks, 1, edges), i32),
            pltpu.VMEM((came, 128), i32),
            pltpu.VMEM((came, width), bf16),
            pltpu.VMEM((came, width), bf16),
            pltpu.VMEM((came, width), bf16),
            pltpu.VMEM((node_rows, width), bf16),
            pltpu.VMEM((8, 128), i32),
            pltpu.SMEM((8, 128), i32),
            pltpu.SemaphoreType.DMA,
            pltpu.SemaphoreType.DMA((2, peers)),
            pltpu.SemaphoreType.DMA((2, peers)),
            pltpu.SemaphoreType.DMA((2, 4, most)),
            pltpu.SemaphoreType.DMA((2, 4, most)),
        ],
        compiler_params=pltpu.CompilerParams(
            collective_id=0, has_side_effects=True, vmem_limit_bytes=VMEM_LIMIT
        ),
        name="rgcn",
    )(
        edge_source[0],
        edge_relation[0],
        edge_target[0],
        send_list[0],
        block_count,
        features,
        bases_first,
        self_first,
        bases_second,
        self_second,
        coef_first,
        coef_second,
        bias_first[None],
        bias_second[None],
    )


def solution(mesh):
    placed = (
        P("dom", None),
        P("dom", None, None),
        P("dom", None, None),
        P("dom", None, None),
        P("dom"),
        P("dom", None, None),
        P(None, "dom", None),
        P("dom", None),
        P(),
        P(),
        P(None, "dom", None),
        P("dom", None),
        P(),
        P(),
    )
    return jax.shard_map(
        functools.partial(shards, mesh.shape["dom"]),
        mesh=mesh,
        in_specs=placed,
        out_specs=P("dom", None),
        check_vma=False,
    )
```

```python
import functools
import math

import jax
import jax.numpy as jnp
from jax import lax
from jax.experimental import pallas as pl
from jax.experimental.pallas import tpu as pltpu
from jax.sharding import PartitionSpec as P

WIN = 16
POOL, COUNT, SPREAD = 16, 32, 16
VMEM_LIMIT = 63 * 1024 * 1024
MESH = pl.DeviceIdType.MESH


def sides(devices):
    chips = devices // 2
    side = max(math.isqrt(chips // 4), 1)
    return chips // (side * side), side, side, 2


def group_of(depth):
    group = 32
    while group * depth > 32 * 1024:
        group //= 2
    return group


def one_hot(columns, first, count):
    lanes = lax.broadcasted_iota(jnp.int32, columns.shape, 1)
    parts = [
        (columns == lanes + (first + part * 128)).astype(jnp.float32).astype(jnp.bfloat16)
        for part in range(count // 128)
    ]
    return jnp.concatenate(parts, axis=1)


def fused_kernel(
    devices,
    source_ref,
    relation_ref,
    target_ref,
    send_ref,
    count_ref,
    features_ref,
    bases_a,
    self_a,
    bases_b,
    self_b,
    coef_a,
    coef_b,
    bias_a,
    bias_b,
    out_ref,
    column_ref,
    picked_ref,
    pooled_ref,
    inverse_ref,
    mean_ref,
    weight_ref,
    pieces_a,
    pieces_b,
    slot_ref,
    send_column_ref,
    sent,
    came_a,
    came_b,
    hidden_ref,
    plan_ref,
    plan_smem,
    plan_sem,
    send_sems,
    recv_sems,
    piece_send_sems,
    piece_recv_sems,
):
    me = lax.axis_index("dom")
    planes, rows_y, rows_x, cores = sides(devices)
    low = rows_y * rows_x * cores
    my_z, my_low = me // low, me % low
    my_y = my_low // (rows_x * cores)
    my_x = my_low // cores % rows_x
    my_core = my_low % cores
    node_rows, width = features_ref.shape
    blocks, edges = source_ref.shape
    peers, slots = send_ref.shape
    relations, bases = coef_a.shape
    share = self_a.shape[0]
    windows = node_rows // WIN
    places = WIN * relations
    plane_rows = low * slots

    def at(z, y, x, core):
        return ((z * rows_y + y) * rows_x + x) * cores + core

    barrier = pltpu.get_barrier_semaphore()

    def greet(hop, carry):
        peer = lax.rem(me + hop, devices)
        pl.semaphore_signal(barrier, inc=1, device_id=(peer,), device_id_type=MESH)
        return carry

    lax.fori_loop(1, devices, greet, 0)

    def compose(bases_ref, self_ref, coef_ref, pieces):
        sums = [jnp.zeros((share, width), jnp.float32) for _ in range(relations)]
        for basis in range(bases):
            matrix = bases_ref[basis].astype(jnp.float32)
            sums = [
                total + coef_ref[relation, basis] * matrix for relation, total in enumerate(sums)
            ]
        for relation, total in enumerate(sums):
            pieces[my_z, my_y, my_x, my_core, relation] = total.astype(jnp.bfloat16)
        pieces[my_z, my_y, my_x, my_core, relations] = self_ref[...]

    compose(bases_a, self_a, coef_a, pieces_a)

    lane_ids = lax.broadcasted_iota(jnp.int32, (edges, 128), 1)
    row_ids = lax.broadcasted_iota(jnp.int32, (edges, 128), 0)
    eye = row_ids == lane_ids
    eye_send = lax.broadcasted_iota(jnp.int32, (slots, slots), 0) == lax.broadcasted_iota(
        jnp.int32, (slots, slots), 1
    )

    def send_columns(group, carry):
        listed = send_ref[pl.ds(pl.multiple_of(group * 8, 8), 8), :]
        for row in range(8):
            spread = jnp.where(eye_send, listed[row : row + 1, :], 0).astype(jnp.float32)
            column = jnp.sum(spread, axis=1, keepdims=True)
            first = pl.multiple_of((group * 8 + row) * slots, slots)
            send_column_ref[pl.ds(first, slots), :] = jnp.broadcast_to(
                column, (slots, 128)
            ).astype(jnp.int32)
        return carry

    lax.fori_loop(0, peers // 8, send_columns, 0)

    def plan():
        window_c = jnp.broadcast_to(target_ref[:, 0:1] // WIN, (blocks, 128))
        window_r = jnp.sum(jnp.where(eye, window_c, 0), axis=0, keepdims=True)
        key_c = window_c * blocks + row_ids
        key_r = window_r * blocks + lane_ids[0:1]
        before = jnp.where(key_c < key_r, 1, 0)
        rank_r = jnp.sum(before, axis=0, keepdims=True)
        same = jnp.where(window_c == window_r, before, 0)
        follows_r = jnp.minimum(jnp.sum(same, axis=0, keepdims=True), 1)
        rank_c = jnp.transpose(jnp.broadcast_to(rank_r, (128, 128)))
        follows_c = jnp.transpose(jnp.broadcast_to(follows_r, (128, 128)))
        placed = rank_c == lane_ids
        order = jnp.sum(jnp.where(placed, row_ids, 0), axis=0, keepdims=True)
        keep = jnp.sum(jnp.where(placed, follows_c, 0), axis=0, keepdims=True)
        last = jnp.max(
            jnp.where(window_c == lane_ids, rank_c + 1, 0), axis=0, keepdims=True
        )
        plan_ref[...] = jnp.concatenate(
            [order, keep, last, jnp.zeros((5, 128), jnp.int32)], axis=0
        )

    plan()

    slot = relation_ref[...] * WIN + target_ref[...] % WIN
    slot_ref[...] = jnp.where(row_ids < count_ref[0], slot, -1).reshape(blocks, 1, edges)

    def copies(layer, stage):
        pieces = (pieces_a, pieces_b)[layer]
        made = []
        if stage == 0:
            count, source = planes, lambda: pieces.at[my_z, my_y, my_x, my_core]
        elif stage == 1:
            count, source = rows_y, lambda: pieces.at[:, my_y, my_x, my_core]
        elif stage == 2:
            count, source = rows_x, lambda: pieces.at[:, :, my_x, my_core]
        else:
            count, source = cores, lambda: pieces.at[:, :, :, my_core]
        for hop in range(1, count):
            to = [my_z, my_y, my_x, my_core]
            to[stage] = lax.rem(to[stage] + hop, count)
            by = [my_z, my_y, my_x, my_core]
            by[stage] = lax.rem(by[stage] + count - hop, count)
            landed = pieces.at[(*(slice(None),) * stage, by[stage], *by[stage + 1 :])]
            if stage == 0:
                landed = pieces.at[by[0], my_y, my_x, my_core]
            pair = (layer, stage, hop)
            sems = dict(
                send_sem=piece_send_sems.at[pair],
                recv_sem=piece_recv_sems.at[pair],
                device_id=(at(*to),),
                device_id_type=MESH,
            )
            made.append(
                (
                    pltpu.make_async_remote_copy(src_ref=source(), dst_ref=source(), **sems),
                    pltpu.make_async_remote_copy(src_ref=landed, dst_ref=landed, **sems),
                )
            )
        return made

    def send_pieces(layer, stage):
        for out, _ in copies(layer, stage):
            out.start()

    def land_pieces(layer, stage):
        for out, landed in copies(layer, stage):
            out.wait_send()
            landed.wait_recv()

    def join_pieces(layer):
        pieces = (pieces_a, pieces_b)[layer]

        group = max(16 // share, 1)
        height = group * share

        def join(step, carry):
            for relation in range(relations + 1):
                rows = []
                for part in range(group):
                    device = step * group + part
                    z, rest = device // low, device % low
                    y, rest = rest // (rows_x * cores), rest % (rows_x * cores)
                    rows.append(
                        pieces[z, y, rest // cores, rest % cores, relation].astype(jnp.float32)
                    )
                first = pl.multiple_of(step * height, height)
                weight_ref[relation, pl.ds(first, height), :] = (
                    rows[0] if group == 1 else jnp.concatenate(rows, axis=0)
                ).astype(jnp.bfloat16)
            return carry

        lax.fori_loop(0, devices // group, join, 0)

    def peer_of(hop_z, hop_low, sign):
        z = lax.rem(my_z + planes + sign * hop_z, planes)
        rest = lax.rem(my_low + low + sign * hop_low, low)
        return z * low + rest

    def row_copy(layer, hop_z, hop_low, landing):
        came = (came_a, came_b)[layer]
        hop = hop_z * low + hop_low
        to = peer_of(hop_z, hop_low, 1)
        owner = peer_of(hop_z, hop_low, -1) if landing else me
        return pltpu.make_async_remote_copy(
            src_ref=sent.at[pl.ds(pl.multiple_of(to * slots, slots), slots)],
            dst_ref=came.at[pl.ds(pl.multiple_of(owner * slots, slots), slots)],
            send_sem=send_sems.at[layer, hop],
            recv_sem=recv_sems.at[layer, hop],
            device_id=(to,),
            device_id_type=MESH,
        )

    def plane_order():
        return sorted(range(planes), key=lambda hop: -min(hop, planes - hop))

    def pick_plane(layer, rows_ref, hop_z):
        z = lax.rem(my_z + hop_z, planes)
        for part in range(plane_rows // 256):
            first = pl.multiple_of(z * plane_rows + part * 256, 256)
            hot = one_hot(send_column_ref[pl.ds(first, 256), :], 0, node_rows)
            sent[pl.ds(first, 256), :] = jnp.dot(
                hot, rows_ref[...], preferred_element_type=jnp.float32
            ).astype(jnp.bfloat16)

    def start_plane(layer, hop_z):
        def start(hop_low, carry):
            row_copy(layer, hop_z, hop_low, False).start()
            return carry

        lax.fori_loop(1 if hop_z == 0 else 0, low, start, 0)

    def land_plane(layer, hop_z):
        def land(hop_low, carry):
            row_copy(layer, hop_z, hop_low, False).wait_send()
            row_copy(layer, hop_z, hop_low, True).wait_recv()
            return carry

        lax.fori_loop(1 if hop_z == 0 else 0, low, land, 0)

    place_ids = lax.broadcasted_iota(jnp.int32, (places, edges), 0)

    def send_rows(layer, rows_ref):
        came = (came_a, came_b)[layer]
        came[pl.ds(pl.multiple_of(me * slots, slots), slots), :] = jnp.zeros(
            (slots, width), jnp.bfloat16
        )
        waiting = None
        for hop_z in plane_order():
            pick_plane(layer, rows_ref, hop_z)
            if waiting is not None:
                start_plane(layer, waiting)
            waiting = hop_z
        return waiting

    def own_stage(rows_ref):
        group = group_of(node_rows)

        def pick(step, carry):
            part = pl.ds(step * group, group)
            hot = one_hot(column_ref[part].reshape(group * edges, 128), 0, node_rows)
            picked_ref[part] = (
                jnp.dot(hot, rows_ref[...], preferred_element_type=jnp.float32)
                .astype(jnp.bfloat16)
                .reshape(group, edges, width)
            )
            return carry

        lax.fori_loop(0, blocks // group, pick, 0)

    def plane_parts(layer, columns, hops):
        came = (came_a, came_b)[layer]
        total = None
        for hop_z in hops:
            z = lax.rem(my_z + planes - hop_z, planes)
            hot = one_hot(columns, node_rows + z * plane_rows, plane_rows)
            rows = came[pl.ds(pl.multiple_of(z * plane_rows, plane_rows), plane_rows), :]
            part = jnp.dot(hot, rows, preferred_element_type=jnp.float32)
            total = part if total is None else total + part
        return total.astype(jnp.bfloat16)

    def near_stage(layer, hops):
        group = group_of(plane_rows * len(hops))

        def pick(step, carry):
            part = pl.ds(step * group, group)
            columns = column_ref[part].reshape(group * edges, 128)
            picked_ref[part] += plane_parts(layer, columns, hops).reshape(group, edges, width)
            return carry

        lax.fori_loop(0, blocks // group, pick, 0)

    def block_at(step):
        return jnp.clip(plan_smem[0, step], 0, blocks - 1)

    def last_of(window):
        return jnp.clip(plan_smem[2, window], 0, blocks)

    def hot_of(block):
        return (place_ids == slot_ref[block]).astype(jnp.float32).astype(jnp.bfloat16)

    def pool_stage(first, count):
        def pool(step, carry):
            total = pooled_ref[step * POOL]
            for part in range(POOL):
                block = block_at(step * POOL + part)
                sums = jnp.dot(
                    hot_of(block), picked_ref[block], preferred_element_type=jnp.float32
                )
                keep = plan_smem[1, step * POOL + part].astype(jnp.float32)
                total = total * keep + sums
                pooled_ref[step * POOL + part + 1] = total
            return carry

        steps = blocks // POOL
        lax.fori_loop(first * steps // 4, (first + count) * steps // 4, pool, 0)

    def degree_stage():
        ones = jnp.ones((edges, 128), jnp.bfloat16)

        def pool(step, carry):
            total = pooled_ref[step * COUNT, :, 0:128]
            for part in range(COUNT):
                block = block_at(step * COUNT + part)
                numbers = jnp.dot(hot_of(block), ones, preferred_element_type=jnp.float32)
                keep = plan_smem[1, step * COUNT + part].astype(jnp.float32)
                total = total * keep + numbers
                pooled_ref[step * COUNT + part + 1, :, 0:128] = total
            return carry

        lax.fori_loop(0, blocks // COUNT, pool, 0)

        def invert(step, carry):
            for part in range(4):
                window = step * 4 + part
                numbers = pooled_ref[last_of(window), :, 0:128]
                inverse_ref[window] = 1.0 / jnp.maximum(numbers, 1.0)
            return carry

        lax.fori_loop(0, windows // 4, invert, 0)

    def mean_stage():
        def average(step, carry):
            for window in [step * 4 + part for part in range(4)]:
                block = last_of(window)
                first = pl.multiple_of(window * WIN, WIN)
                for relation in range(relations):
                    part = slice(relation * WIN, (relation + 1) * WIN)
                    inverse = inverse_ref[window, part, :]
                    for lane in range(0, width, 128):
                        mean_ref[relation, pl.ds(first, WIN), lane : lane + 128] = (
                            pooled_ref[block, part, lane : lane + 128] * inverse
                        ).astype(jnp.bfloat16)
            return carry

        lax.fori_loop(0, windows // 4, average, 0)

    def dense_stage(rows_ref, bias_ref, result_ref, last):
        def dense(chunk, carry):
            rows = pl.ds(pl.multiple_of(chunk * 512, 512), 512)
            total = bias_ref[...] + jnp.dot(
                rows_ref[rows, :], weight_ref[relations], preferred_element_type=jnp.float32
            )
            for relation in range(relations):
                total = total + jnp.dot(
                    mean_ref[relation, rows, :],
                    weight_ref[relation],
                    preferred_element_type=jnp.float32,
                )
            if not last:
                total = jnp.maximum(total, 0.0)
            result_ref[rows, :] = total.astype(jnp.bfloat16)
            return carry

        lax.fori_loop(0, node_rows // 512, dense, 0)

    def source_columns():
        turned = jnp.transpose(source_ref[...].astype(jnp.float32))
        ones_wide = jnp.ones((2 * edges, 128), jnp.bfloat16)

        def spread(group, carry):
            rolled = pltpu.roll(turned, blocks - group * SPREAD, 1)
            listed = source_ref[pl.ds(pl.multiple_of(group * SPREAD, SPREAD), SPREAD), :]
            small = listed % 128
            large = (listed - small).astype(jnp.float32)
            small = small.astype(jnp.float32)
            for row in range(SPREAD):
                if row % 2:
                    column = jnp.broadcast_to(rolled[:, row : row + 1], (edges, 128))
                else:
                    diagonal = [
                        jnp.where(eye, one[row : row + 1, :], 0.0).astype(jnp.bfloat16)
                        for one in (large, small)
                    ]
                    column = jnp.dot(
                        jnp.concatenate(diagonal, axis=1),
                        ones_wide,
                        preferred_element_type=jnp.float32,
                    )
                column_ref[group * SPREAD + row] = column.astype(jnp.int32)
            return carry

        lax.fori_loop(0, blocks // SPREAD, spread, 0)

    near = [planes // 2]
    far = [hop for hop in range(planes) if hop not in near]

    scope = jax.named_scope
    plan_copy = pltpu.make_async_copy(plan_ref, plan_smem, plan_sem)
    plan_copy.start()
    pooled_ref[0] = jnp.zeros(pooled_ref.shape[1:], jnp.float32)
    with scope("columns"):
        source_columns()
    with scope("greeted"):
        pl.semaphore_wait(barrier, devices - 1)
    send_pieces(0, 0)
    with scope("send_a"):
        waiting = send_rows(0, features_ref)
    plan_copy.wait()
    with scope("compose_b"):
        compose(bases_b, self_b, coef_b, pieces_b)
    start_plane(0, waiting)
    with scope("degree"):
        degree_stage()
    with scope("own_a"):
        own_stage(features_ref)
    with scope("piece_z"):
        land_pieces(0, 0)
    send_pieces(0, 1)
    with scope("land_near_a"):
        for hop in near:
            land_plane(0, hop)
    with scope("near_a"):
        near_stage(0, near)
    with scope("land_far_a"):
        for hop in far:
            land_plane(0, hop)
    with scope("piece_y"):
        land_pieces(0, 1)
    send_pieces(0, 2)
    send_pieces(1, 0)
    with scope("far_a"):
        near_stage(0, far)
    with scope("pool_a1"):
        pool_stage(0, 2)
    with scope("piece_x"):
        land_pieces(0, 2)
    send_pieces(0, 3)
    with scope("pool_a2"):
        pool_stage(2, 2)
    with scope("piece_z_b"):
        land_pieces(1, 0)
    send_pieces(1, 1)
    with scope("mean_a"):
        mean_stage()
    with scope("piece_core"):
        land_pieces(0, 3)
    with scope("join_a"):
        join_pieces(0)
    with scope("dense_a"):
        dense_stage(features_ref, bias_a, hidden_ref, False)

    with scope("send_b"):
        waiting = send_rows(1, hidden_ref)
    with scope("piece_y_b"):
        land_pieces(1, 1)
    start_plane(1, waiting)
    send_pieces(1, 2)
    with scope("own_b"):
        own_stage(hidden_ref)
    with scope("land_near_b"):
        for hop in near:
            land_plane(1, hop)
    with scope("near_b"):
        near_stage(1, near)
    with scope("piece_x_b"):
        land_pieces(1, 2)
    send_pieces(1, 3)
    with scope("land_far_b"):
        for hop in far:
            land_plane(1, hop)
    with scope("far_b"):
        near_stage(1, far)
    with scope("pool_b"):
        pool_stage(0, 4)
    with scope("mean_b"):
        mean_stage()
    with scope("piece_core_b"):
        land_pieces(1, 3)
    with scope("join_b"):
        join_pieces(1)
    with scope("dense_b"):
        dense_stage(hidden_ref, bias_b, out_ref, True)


def in_smem():
    return pl.BlockSpec(memory_space=pltpu.SMEM)


def in_vmem():
    return pl.BlockSpec(memory_space=pltpu.VMEM)


def shards(
    devices,
    features,
    edge_source,
    edge_relation,
    edge_target,
    block_count,
    send_list,
    bases_first,
    self_first,
    coef_first,
    bias_first,
    bases_second,
    self_second,
    coef_second,
    bias_second,
):
    node_rows, width = features.shape
    _, blocks, edges = edge_source.shape
    _, peers, slots = send_list.shape
    relations = coef_first.shape[0]
    share = self_first.shape[0]
    planes, rows_y, rows_x, cores = sides(devices)
    windows = node_rows // WIN
    places = WIN * relations
    came = peers * slots
    bf16, f32, i32 = jnp.bfloat16, jnp.float32, jnp.int32
    piece = (planes, rows_y, rows_x, cores, relations + 1, share, width)
    most = max(planes, rows_y, rows_x, cores)
    return pl.pallas_call(
        functools.partial(fused_kernel, devices),
        out_shape=jax.ShapeDtypeStruct((node_rows, width), bf16),
        in_specs=[in_vmem()] * 4
        + [in_smem()]
        + [in_vmem()] * 5
        + [in_smem()] * 2
        + [in_vmem()] * 2,
        out_specs=in_vmem(),
        scratch_shapes=[
            pltpu.VMEM((blocks, edges, 128), i32),
            pltpu.VMEM((blocks, edges, width), bf16),
            pltpu.VMEM((blocks + 1, places, width), f32),
            pltpu.VMEM((windows, places, 128), f32),
            pltpu.VMEM((relations, node_rows, width), bf16),
            pltpu.VMEM((relations + 1, width, width), bf16),
            pltpu.VMEM(piece, bf16),
            pltpu.VMEM(piece, bf16),
            pltpu.VMEM((blocks, 1, edges), i32),
            pltpu.VMEM((came, 128), i32),
            pltpu.VMEM((came, width), bf16),
            pltpu.VMEM((came, width), bf16),
            pltpu.VMEM((came, width), bf16),
            pltpu.VMEM((node_rows, width), bf16),
            pltpu.VMEM((8, 128), i32),
            pltpu.SMEM((8, 128), i32),
            pltpu.SemaphoreType.DMA,
            pltpu.SemaphoreType.DMA((2, peers)),
            pltpu.SemaphoreType.DMA((2, peers)),
            pltpu.SemaphoreType.DMA((2, 4, most)),
            pltpu.SemaphoreType.DMA((2, 4, most)),
        ],
        compiler_params=pltpu.CompilerParams(
            collective_id=0, has_side_effects=True, vmem_limit_bytes=VMEM_LIMIT
        ),
        name="rgcn",
    )(
        edge_source[0],
        edge_relation[0],
        edge_target[0],
        send_list[0],
        block_count,
        features,
        bases_first,
        self_first,
        bases_second,
        self_second,
        coef_first,
        coef_second,
        bias_first[None],
        bias_second[None],
    )


def solution(mesh):
    placed = (
        P("dom", None),
        P("dom", None, None),
        P("dom", None, None),
        P("dom", None, None),
        P("dom"),
        P("dom", None, None),
        P(None, "dom", None),
        P("dom", None),
        P(),
        P(),
        P(None, "dom", None),
        P("dom", None),
        P(),
        P(),
    )
    return jax.shard_map(
        functools.partial(shards, mesh.shape["dom"]),
        mesh=mesh,
        in_specs=placed,
        out_specs=P("dom", None),
        check_vma=False,
    )
```

```python
import functools
import math

import jax
import jax.numpy as jnp
from jax import lax
from jax.experimental import pallas as pl
from jax.experimental.pallas import tpu as pltpu
from jax.sharding import PartitionSpec as P

WIN = 16
POOL, COUNT = 32, 32
VMEM_LIMIT = 63 * 1024 * 1024
MESH = pl.DeviceIdType.MESH


def sides(devices):
    chips = devices // 2
    side = max(math.isqrt(chips // 4), 1)
    return chips // (side * side), side, side, 2


def group_of(depth, devices):
    group = 32
    while group * depth * devices > 1024 * 1024:
        group //= 2
    return group


def one_hot(columns, first, count):
    lanes = lax.broadcasted_iota(jnp.int32, columns.shape, 1)
    parts = [
        (columns == lanes + (first + part * 128)).astype(jnp.float32).astype(jnp.bfloat16)
        for part in range(count // 128)
    ]
    return jnp.concatenate(parts, axis=1)


def fused_kernel(
    devices,
    source_ref,
    relation_ref,
    target_ref,
    send_ref,
    count_ref,
    features_ref,
    bases_a,
    self_a,
    bases_b,
    self_b,
    coef_a,
    coef_b,
    bias_a,
    bias_b,
    out_ref,
    column_ref,
    picked_ref,
    pooled_ref,
    inverse_ref,
    mean_ref,
    weight_ref,
    pieces_a,
    pieces_b,
    slot_ref,
    send_column_ref,
    sent,
    came_a,
    came_b,
    plan_ref,
    turned_ref,
    plan_smem,
    plan_sem,
    send_sems,
    recv_sems,
    piece_send_sems,
    piece_recv_sems,
):
    me = lax.axis_index("dom")
    planes, rows_y, rows_x, cores = sides(devices)
    low = rows_y * rows_x * cores
    my_z, my_low = me // low, me % low
    my_y = my_low // (rows_x * cores)
    my_x = my_low // cores % rows_x
    my_core = my_low % cores
    node_rows, width = features_ref.shape
    blocks, edges = source_ref.shape
    peers, slots = send_ref.shape
    relations, bases = coef_a.shape
    share = self_a.shape[0]
    windows = node_rows // WIN
    places = WIN * relations
    plane_rows = low * slots

    def at(z, y, x, core):
        return ((z * rows_y + y) * rows_x + x) * cores + core

    barrier = pltpu.get_barrier_semaphore()

    def greet(hop, carry):
        peer = lax.rem(me + hop, devices)
        pl.semaphore_signal(barrier, inc=1, device_id=(peer,), device_id_type=MESH)
        return carry

    lax.fori_loop(1, devices, greet, 0)

    def compose(bases_ref, self_ref, coef_ref, pieces):
        sums = [jnp.zeros((share, width), jnp.float32) for _ in range(relations)]
        for basis in range(bases):
            matrix = bases_ref[basis].astype(jnp.float32)
            sums = [
                total + coef_ref[relation, basis] * matrix for relation, total in enumerate(sums)
            ]
        for relation, total in enumerate(sums):
            pieces[my_z, my_y, my_x, my_core, relation] = total.astype(jnp.bfloat16)
        pieces[my_z, my_y, my_x, my_core, relations] = self_ref[...]

    compose(bases_a, self_a, coef_a, pieces_a)

    lane_ids = lax.broadcasted_iota(jnp.int32, (edges, 128), 1)
    row_ids = lax.broadcasted_iota(jnp.int32, (edges, 128), 0)
    eye = row_ids == lane_ids
    eye_send = lax.broadcasted_iota(jnp.int32, (slots, slots), 0) == lax.broadcasted_iota(
        jnp.int32, (slots, slots), 1
    )

    def send_columns(group, carry):
        listed = send_ref[pl.ds(pl.multiple_of(group * 8, 8), 8), :]
        for row in range(8):
            spread = jnp.where(eye_send, listed[row : row + 1, :], 0).astype(jnp.float32)
            column = jnp.sum(spread, axis=1, keepdims=True)
            first = pl.multiple_of((group * 8 + row) * slots, slots)
            send_column_ref[pl.ds(first, slots), :] = jnp.broadcast_to(
                column, (slots, 128)
            ).astype(jnp.int32)
        return carry

    lax.fori_loop(0, peers // 8, send_columns, 0)

    def plan():
        window_c = jnp.broadcast_to(target_ref[:, 0:1] // WIN, (blocks, 128))
        window_r = jnp.sum(jnp.where(eye, window_c, 0), axis=0, keepdims=True)
        key_c = window_c * blocks + row_ids
        key_r = window_r * blocks + lane_ids[0:1]
        before = jnp.where(key_c < key_r, 1, 0)
        rank_r = jnp.sum(before, axis=0, keepdims=True)
        same = jnp.where(window_c == window_r, before, 0)
        follows_r = jnp.minimum(jnp.sum(same, axis=0, keepdims=True), 1)
        rank_c = jnp.transpose(jnp.broadcast_to(rank_r, (128, 128)))
        follows_c = jnp.transpose(jnp.broadcast_to(follows_r, (128, 128)))
        placed = rank_c == lane_ids
        order = jnp.sum(jnp.where(placed, row_ids, 0), axis=0, keepdims=True)
        keep = jnp.sum(jnp.where(placed, follows_c, 0), axis=0, keepdims=True)
        last = jnp.max(
            jnp.where(window_c == lane_ids, rank_c + 1, 0), axis=0, keepdims=True
        )
        plan_ref[...] = jnp.concatenate(
            [order, keep, last, jnp.zeros((5, 128), jnp.int32)], axis=0
        )

    plan()

    slot = relation_ref[...] * WIN + target_ref[...] % WIN
    slot_ref[...] = jnp.where(row_ids < count_ref[0, 0], slot, -1).reshape(blocks, 1, edges)

    def copies(layer, stage):
        pieces = (pieces_a, pieces_b)[layer]
        made = []
        if stage == 0:
            count, source = planes, lambda: pieces.at[my_z, my_y, my_x, my_core]
        elif stage == 1:
            count, source = rows_y, lambda: pieces.at[:, my_y, my_x, my_core]
        elif stage == 2:
            count, source = rows_x, lambda: pieces.at[:, :, my_x, my_core]
        else:
            count, source = cores, lambda: pieces.at[:, :, :, my_core]
        for hop in range(1, count):
            to = [my_z, my_y, my_x, my_core]
            to[stage] = lax.rem(to[stage] + hop, count)
            by = [my_z, my_y, my_x, my_core]
            by[stage] = lax.rem(by[stage] + count - hop, count)
            landed = pieces.at[(*(slice(None),) * stage, by[stage], *by[stage + 1 :])]
            if stage == 0:
                landed = pieces.at[by[0], my_y, my_x, my_core]
            pair = (layer, stage, hop)
            sems = dict(
                send_sem=piece_send_sems.at[pair],
                recv_sem=piece_recv_sems.at[pair],
                device_id=(at(*to),),
                device_id_type=MESH,
            )
            made.append(
                (
                    pltpu.make_async_remote_copy(src_ref=source(), dst_ref=source(), **sems),
                    pltpu.make_async_remote_copy(src_ref=landed, dst_ref=landed, **sems),
                )
            )
        return made

    def send_pieces(layer, stage):
        for out, _ in copies(layer, stage):
            out.start()

    def land_pieces(layer, stage):
        for out, landed in copies(layer, stage):
            out.wait_send()
            landed.wait_recv()

    def join_pieces(layer):
        pieces = (pieces_a, pieces_b)[layer]

        group = max(16 // share, 1)
        height = group * share

        def join(step, carry):
            for relation in range(relations + 1):
                rows = []
                for part in range(group):
                    device = step * group + part
                    z, rest = device // low, device % low
                    y, rest = rest // (rows_x * cores), rest % (rows_x * cores)
                    rows.append(
                        pieces[z, y, rest // cores, rest % cores, relation].astype(jnp.float32)
                    )
                first = pl.multiple_of(step * height, height)
                weight_ref[relation, pl.ds(first, height), :] = (
                    rows[0] if group == 1 else jnp.concatenate(rows, axis=0)
                ).astype(jnp.bfloat16)
            return carry

        lax.fori_loop(0, devices // group, join, 0)

    def peer_of(hop_z, hop_low, sign):
        z = lax.rem(my_z + planes + sign * hop_z, planes)
        rest = lax.rem(my_low + low + sign * hop_low, low)
        return z * low + rest

    def row_copy(layer, hop_z, hop_low, landing):
        came = (came_a, came_b)[layer]
        hop = hop_z * low + hop_low
        to = peer_of(hop_z, hop_low, 1)
        owner = peer_of(hop_z, hop_low, -1) if landing else me
        return pltpu.make_async_remote_copy(
            src_ref=sent.at[pl.ds(pl.multiple_of(to * slots, slots), slots)],
            dst_ref=came.at[pl.ds(pl.multiple_of(owner * slots, slots), slots)],
            send_sem=send_sems.at[layer, hop],
            recv_sem=recv_sems.at[layer, hop],
            device_id=(to,),
            device_id_type=MESH,
        )

    def plane_order():
        order = sorted(range(planes), key=lambda hop: -min(hop, planes - hop))
        return order[:1] + [0] * (planes > 1) + order[1:-1]

    def pick_plane(layer, rows_ref, hop_z):
        z = lax.rem(my_z + hop_z, planes)
        for part in range(plane_rows // 256):
            first = pl.multiple_of(z * plane_rows + part * 256, 256)
            hot = one_hot(send_column_ref[pl.ds(first, 256), :], 0, node_rows)
            sent[pl.ds(first, 256), :] = jnp.dot(
                hot, rows_ref[...], preferred_element_type=jnp.float32
            ).astype(jnp.bfloat16)

    def start_plane(layer, hop_z):
        def start(hop_low, carry):
            row_copy(layer, hop_z, hop_low, False).start()
            return carry

        lax.fori_loop(1 if hop_z == 0 else 0, low, start, 0)

    def land_plane(layer, hop_z):
        def land(hop_low, carry):
            row_copy(layer, hop_z, hop_low, False).wait_send()
            row_copy(layer, hop_z, hop_low, True).wait_recv()
            return carry

        lax.fori_loop(1 if hop_z == 0 else 0, low, land, 0)

    place_ids = lax.broadcasted_iota(jnp.int32, (places, edges), 0)

    def send_rows(layer, rows_ref):
        came = (came_a, came_b)[layer]
        came[pl.ds(pl.multiple_of(me * slots, slots), slots), :] = jnp.zeros(
            (slots, width), jnp.bfloat16
        )
        waiting = None
        for hop_z in plane_order():
            pick_plane(layer, rows_ref, hop_z)
            if waiting is not None:
                start_plane(layer, waiting)
            waiting = hop_z
        return waiting

    def own_stage(rows_ref, spreading, between=None):
        group = group_of(node_rows, devices)

        def pick(step, first):
            part = pl.ds(first, group)
            hot = one_hot(column_ref[part].reshape(group * edges, 128), 0, node_rows)
            picked_ref[part] = (
                jnp.dot(hot, rows_ref[...], preferred_element_type=jnp.float32)
                .astype(jnp.bfloat16)
                .reshape(group, edges, width)
            )

        if spreading:
            group = min(group, 16)
            source_columns(0, group, True)
            for first in range(0, blocks, group):
                if first + group < blocks:
                    source_columns(first + group, group, False)
                pick(0, first)
                if between is not None and (first + group) * 4 == blocks * 3:
                    between()
        else:

            def body(step, carry):
                pick(step, step * group)
                return carry

            lax.fori_loop(0, blocks // group, body, 0)

    def plane_parts(layer, columns, hops):
        came = (came_a, came_b)[layer]
        total = None
        for hop_z in hops:
            z = lax.rem(my_z + planes - hop_z, planes)
            hot = one_hot(columns, node_rows + z * plane_rows, plane_rows)
            rows = came[pl.ds(pl.multiple_of(z * plane_rows, plane_rows), plane_rows), :]
            part = jnp.dot(hot, rows, preferred_element_type=jnp.float32)
            total = part if total is None else total + part
        return total.astype(jnp.bfloat16)

    def near_stage(layer, hops):
        group = group_of(plane_rows * len(hops), devices)

        def pick(step, carry):
            part = pl.ds(step * group, group)
            columns = column_ref[part].reshape(group * edges, 128)
            picked_ref[part] += plane_parts(layer, columns, hops).reshape(group, edges, width)
            return carry

        lax.fori_loop(0, blocks // group, pick, 0)

    def block_at(step):
        return jnp.clip(plan_smem[0, step], 0, blocks - 1)

    def last_of(window):
        return jnp.clip(plan_smem[2, window], 0, blocks)

    def hot_of(block):
        return (place_ids == slot_ref[block]).astype(jnp.float32).astype(jnp.bfloat16)

    def pool_stage(first, count):
        def pool(step, carry):
            total = pooled_ref[step * POOL]
            for part in range(POOL):
                block = block_at(step * POOL + part)
                sums = jnp.dot(
                    hot_of(block), picked_ref[block], preferred_element_type=jnp.float32
                )
                keep = plan_smem[1, step * POOL + part].astype(jnp.float32)
                total = total * keep + sums
                pooled_ref[step * POOL + part + 1] = total
            return carry

        steps = blocks // POOL
        lax.fori_loop(first * steps // 4, (first + count) * steps // 4, pool, 0)

    def degree_stage():
        ones = jnp.ones((edges, 128), jnp.bfloat16)

        def pool(step, carry):
            total = pooled_ref[step * COUNT, :, 0:128]
            for part in range(COUNT):
                block = block_at(step * COUNT + part)
                numbers = jnp.dot(hot_of(block), ones, preferred_element_type=jnp.float32)
                keep = plan_smem[1, step * COUNT + part].astype(jnp.float32)
                total = total * keep + numbers
                pooled_ref[step * COUNT + part + 1, :, 0:128] = total
            return carry

        lax.fori_loop(0, blocks // COUNT, pool, 0)

        def invert(step, carry):
            for part in range(4):
                window = step * 4 + part
                numbers = pooled_ref[last_of(window), :, 0:128]
                inverse_ref[window] = 1.0 / jnp.maximum(numbers, 1.0)
            return carry

        lax.fori_loop(0, windows // 4, invert, 0)

    def mean_stage():
        def average(step, carry):
            for window in [step * 4 + part for part in range(4)]:
                block = last_of(window)
                first = pl.multiple_of(window * WIN, WIN)
                for relation in range(relations):
                    part = slice(relation * WIN, (relation + 1) * WIN)
                    inverse = inverse_ref[window, part, :]
                    for lane in range(0, width, 128):
                        mean_ref[relation, pl.ds(first, WIN), lane : lane + 128] = (
                            pooled_ref[block, part, lane : lane + 128] * inverse
                        ).astype(jnp.bfloat16)
            return carry

        lax.fori_loop(0, windows // 4, average, 0)

    def dense_stage(rows_ref, bias_ref, result_ref, last):
        def dense(chunk, carry):
            rows = pl.ds(pl.multiple_of(chunk * 512, 512), 512)
            total = bias_ref[...] + jnp.dot(
                rows_ref[rows, :], weight_ref[relations], preferred_element_type=jnp.float32
            )
            for relation in range(relations):
                total = total + jnp.dot(
                    mean_ref[relation, rows, :],
                    weight_ref[relation],
                    preferred_element_type=jnp.float32,
                )
            if not last:
                total = jnp.maximum(total, 0.0)
            result_ref[rows, :] = total.astype(jnp.bfloat16)
            return carry

        lax.fori_loop(0, node_rows // 512, dense, 0)

    def source_columns(start, count, mixed):
        if mixed:
            ones_wide = jnp.ones((2 * edges, 128), jnp.bfloat16)
        listed = source_ref[start : start + count, :]
        turned = turned_ref[...]
        small = listed % 128
        large = (listed - small).astype(jnp.float32)
        small = small.astype(jnp.float32)
        for row in range(count):
            if row % 2 or not mixed:
                column = jnp.broadcast_to(
                    turned[:, start + row : start + row + 1], (edges, 128)
                )
            else:
                diagonal = [
                    jnp.where(eye, one[row : row + 1, :], 0.0).astype(jnp.bfloat16)
                    for one in (large, small)
                ]
                column = jnp.dot(
                    jnp.concatenate(diagonal, axis=1),
                    ones_wide,
                    preferred_element_type=jnp.float32,
                )
            column_ref[start + row] = column.astype(jnp.int32)

    near = [0]
    far = [hop for hop in plane_order() if hop not in near]

    scope = jax.named_scope
    plan_copy = pltpu.make_async_copy(plan_ref, plan_smem, plan_sem)
    plan_copy.start()
    pooled_ref[0] = jnp.zeros(pooled_ref.shape[1:], jnp.float32)
    turned_ref[...] = jnp.transpose(source_ref[...].astype(jnp.float32))
    plan_copy.wait()
    with scope("degree"):
        degree_stage()
    with scope("greeted"):
        pl.semaphore_wait(barrier, devices - 1)
    send_pieces(0, 0)
    with scope("send_a"):
        waiting = send_rows(0, features_ref)
    with scope("compose_b"):
        compose(bases_b, self_b, coef_b, pieces_b)
    start_plane(0, waiting)

    def forward():
        land_pieces(0, 0)
        send_pieces(0, 1)

    with scope("own_a"):
        own_stage(features_ref, True, forward)
    with scope("land_near_a"):
        for hop in near:
            land_plane(0, hop)
    with scope("near_a"):
        near_stage(0, near)
    with scope("land_mid_a"):
        for hop in far[:1]:
            land_plane(0, hop)
    with scope("mid_a"):
        near_stage(0, far[:1])
    with scope("piece_y"):
        land_pieces(0, 1)
    send_pieces(0, 2)
    send_pieces(1, 0)
    with scope("land_far_a"):
        for hop in far[1:]:
            land_plane(0, hop)
    with scope("far_a"):
        near_stage(0, far[1:])
    with scope("pool_a"):
        pool_stage(0, 4)
    with scope("piece_x"):
        land_pieces(0, 2)
    send_pieces(0, 3)
    with scope("piece_z_b"):
        land_pieces(1, 0)
    send_pieces(1, 1)
    with scope("mean_a"):
        mean_stage()
    with scope("piece_core"):
        land_pieces(0, 3)
    with scope("join_a"):
        join_pieces(0)
    with scope("dense_a"):
        dense_stage(features_ref, bias_a, out_ref, False)

    with scope("send_b"):
        waiting = send_rows(1, out_ref)
    start_plane(1, waiting)
    with scope("piece_y_b"):
        land_pieces(1, 1)
    send_pieces(1, 2)
    with scope("own_b"):
        own_stage(out_ref, False)
    with scope("land_near_b"):
        for hop in near:
            land_plane(1, hop)
    with scope("near_b"):
        near_stage(1, near)
    with scope("piece_x_b"):
        land_pieces(1, 2)
    send_pieces(1, 3)
    with scope("land_far_b"):
        for hop in far:
            land_plane(1, hop)
    with scope("far_b"):
        near_stage(1, far)
    with scope("pool_b"):
        pool_stage(0, 4)
    with scope("mean_b"):
        mean_stage()
    with scope("piece_core_b"):
        land_pieces(1, 3)
    with scope("join_b"):
        join_pieces(1)
    with scope("dense_b"):
        dense_stage(out_ref, bias_b, out_ref, True)


def in_smem():
    return pl.BlockSpec(memory_space=pltpu.SMEM)


def in_vmem():
    return pl.BlockSpec(memory_space=pltpu.VMEM)


def shards(
    devices,
    features,
    edge_source,
    edge_relation,
    edge_target,
    block_count,
    send_list,
    bases_first,
    self_first,
    coef_first,
    bias_first,
    bases_second,
    self_second,
    coef_second,
    bias_second,
):
    node_rows, width = features.shape
    _, blocks, edges = edge_source.shape
    _, peers, slots = send_list.shape
    relations = coef_first.shape[0]
    share = self_first.shape[0]
    planes, rows_y, rows_x, cores = sides(devices)
    windows = node_rows // WIN
    places = WIN * relations
    came = peers * slots
    bf16, f32, i32 = jnp.bfloat16, jnp.float32, jnp.int32
    piece = (planes, rows_y, rows_x, cores, relations + 1, share, width)
    most = max(planes, rows_y, rows_x, cores)
    return pl.pallas_call(
        functools.partial(fused_kernel, devices),
        out_shape=pltpu.VMEM((node_rows, width), bf16),
        in_specs=[in_vmem()] * 4
        + [in_smem()]
        + [in_vmem()] * 5
        + [in_smem()] * 2
        + [in_vmem()] * 2,
        out_specs=in_vmem(),
        scratch_shapes=[
            pltpu.VMEM((blocks, edges, 128), i32),
            pltpu.VMEM((blocks, edges, width), bf16),
            pltpu.VMEM((blocks + 1, places, width), f32),
            pltpu.VMEM((windows, places, 128), f32),
            pltpu.VMEM((relations, node_rows, width), bf16),
            pltpu.VMEM((relations + 1, width, width), bf16),
            pltpu.VMEM(piece, bf16),
            pltpu.VMEM(piece, bf16),
            pltpu.VMEM((blocks, 1, edges), i32),
            pltpu.VMEM((came, 128), i32),
            pltpu.VMEM((came, width), bf16),
            pltpu.VMEM((came, width), bf16),
            pltpu.VMEM((came, width), bf16),
            pltpu.VMEM((8, 128), i32),
            pltpu.VMEM((edges, blocks), f32),
            pltpu.SMEM((8, 128), i32),
            pltpu.SemaphoreType.DMA,
            pltpu.SemaphoreType.DMA((2, peers)),
            pltpu.SemaphoreType.DMA((2, peers)),
            pltpu.SemaphoreType.DMA((2, 4, most)),
            pltpu.SemaphoreType.DMA((2, 4, most)),
        ],
        compiler_params=pltpu.CompilerParams(
            collective_id=0, has_side_effects=True, vmem_limit_bytes=VMEM_LIMIT
        ),
        name="rgcn",
    )(
        edge_source[0],
        edge_relation[0],
        edge_target[0],
        send_list[0],
        block_count[None],
        features,
        bases_first,
        self_first,
        bases_second,
        self_second,
        coef_first,
        coef_second,
        bias_first[None],
        bias_second[None],
    )


def solution(mesh):
    placed = (
        P("dom", None),
        P("dom", None, None),
        P("dom", None, None),
        P("dom", None, None),
        P("dom"),
        P("dom", None, None),
        P(None, "dom", None),
        P("dom", None),
        P(),
        P(),
        P(None, "dom", None),
        P("dom", None),
        P(),
        P(),
    )
    return jax.shard_map(
        functools.partial(shards, mesh.shape["dom"]),
        mesh=mesh,
        in_specs=placed,
        out_specs=P("dom", None),
        check_vma=False,
    )
```

```python
import functools
import math

import jax
import jax.numpy as jnp
from jax import lax
from jax.experimental import pallas as pl
from jax.experimental.pallas import tpu as pltpu
from jax.sharding import PartitionSpec as P

WIN = 16
POOL, COUNT = 32, 32
VMEM_LIMIT = 63 * 1024 * 1024
MESH = pl.DeviceIdType.MESH


def sides(devices):
    chips = devices // 2
    side = max(math.isqrt(chips // 4), 1)
    return chips // (side * side), side, side, 2


def group_of(depth, devices):
    group = 32
    while group * depth * devices > 1024 * 1024:
        group //= 2
    return group


def one_hot(columns, first, count):
    lanes = lax.broadcasted_iota(jnp.int32, columns.shape, 1)
    parts = [
        (columns == lanes + (first + part * 128)).astype(jnp.float32).astype(jnp.bfloat16)
        for part in range(count // 128)
    ]
    return jnp.concatenate(parts, axis=1)


def fused_kernel(
    devices,
    source_ref,
    relation_ref,
    target_ref,
    send_ref,
    count_ref,
    features_ref,
    bases_a,
    self_a,
    bases_b,
    self_b,
    coef_a,
    coef_b,
    bias_a,
    bias_b,
    out_ref,
    column_ref,
    picked_ref,
    pooled_ref,
    inverse_ref,
    mean_ref,
    weight_ref,
    pieces_a,
    pieces_b,
    slot_ref,
    send_column_ref,
    sent,
    came_a,
    came_b,
    plan_ref,
    turned_ref,
    plan_smem,
    plan_sem,
    send_sems,
    recv_sems,
    piece_send_sems,
    piece_recv_sems,
):
    me = lax.axis_index("dom")
    planes, rows_y, rows_x, cores = sides(devices)
    low = rows_y * rows_x * cores
    my_z, my_low = me // low, me % low
    my_y = my_low // (rows_x * cores)
    my_x = my_low // cores % rows_x
    my_core = my_low % cores
    node_rows, width = features_ref.shape
    blocks, edges = source_ref.shape
    peers, slots = send_ref.shape
    relations, bases = coef_a.shape
    share = self_a.shape[0]
    windows = node_rows // WIN
    places = WIN * relations
    plane_rows = low * slots

    def at(z, y, x, core):
        return ((z * rows_y + y) * rows_x + x) * cores + core

    barrier = pltpu.get_barrier_semaphore()

    def greet(hop, carry):
        peer = lax.rem(me + hop, devices)
        pl.semaphore_signal(barrier, inc=1, device_id=(peer,), device_id_type=MESH)
        return carry

    lax.fori_loop(1, devices, greet, 0)

    def compose(bases_ref, self_ref, coef_ref, pieces):
        sums = [jnp.zeros((share, width), jnp.float32) for _ in range(relations)]
        for basis in range(bases):
            matrix = bases_ref[basis].astype(jnp.float32)
            sums = [
                total + coef_ref[relation, basis] * matrix for relation, total in enumerate(sums)
            ]
        for relation, total in enumerate(sums):
            pieces[my_z, my_y, my_x, my_core, relation] = total.astype(jnp.bfloat16)
        pieces[my_z, my_y, my_x, my_core, relations] = self_ref[...]

    compose(bases_a, self_a, coef_a, pieces_a)

    lane_ids = lax.broadcasted_iota(jnp.int32, (edges, 128), 1)
    row_ids = lax.broadcasted_iota(jnp.int32, (edges, 128), 0)
    eye = row_ids == lane_ids
    eye_send = lax.broadcasted_iota(jnp.int32, (slots, slots), 0) == lax.broadcasted_iota(
        jnp.int32, (slots, slots), 1
    )

    def send_columns(group, carry):
        listed = send_ref[pl.ds(pl.multiple_of(group * 8, 8), 8), :]
        for row in range(8):
            spread = jnp.where(eye_send, listed[row : row + 1, :], 0).astype(jnp.float32)
            column = jnp.sum(spread, axis=1, keepdims=True)
            first = pl.multiple_of((group * 8 + row) * slots, slots)
            send_column_ref[pl.ds(first, slots), :] = jnp.broadcast_to(
                column, (slots, 128)
            ).astype(jnp.int32)
        return carry

    lax.fori_loop(0, peers // 8, send_columns, 0)

    def plan():
        window_c = jnp.broadcast_to(target_ref[:, 0:1] // WIN, (blocks, 128))
        window_r = jnp.sum(jnp.where(eye, window_c, 0), axis=0, keepdims=True)
        key_c = window_c * blocks + row_ids
        key_r = window_r * blocks + lane_ids[0:1]
        before = jnp.where(key_c < key_r, 1, 0)
        rank_r = jnp.sum(before, axis=0, keepdims=True)
        same = jnp.where(window_c == window_r, before, 0)
        follows_r = jnp.minimum(jnp.sum(same, axis=0, keepdims=True), 1)
        rank_c = jnp.transpose(jnp.broadcast_to(rank_r, (128, 128)))
        follows_c = jnp.transpose(jnp.broadcast_to(follows_r, (128, 128)))
        placed = rank_c == lane_ids
        order = jnp.sum(jnp.where(placed, row_ids, 0), axis=0, keepdims=True)
        keep = jnp.sum(jnp.where(placed, follows_c, 0), axis=0, keepdims=True)
        last = jnp.max(
            jnp.where(window_c == lane_ids, rank_c + 1, 0), axis=0, keepdims=True
        )
        plan_ref[...] = jnp.concatenate(
            [order, keep, last, jnp.zeros((5, 128), jnp.int32)], axis=0
        )

    plan()

    slot = relation_ref[...] * WIN + target_ref[...] % WIN
    slot_ref[...] = jnp.where(row_ids < count_ref[0, 0], slot, -1).reshape(blocks, 1, edges)

    def copies(layer, stage):
        pieces = (pieces_a, pieces_b)[layer]
        made = []
        if stage == 0:
            count, source = planes, lambda: pieces.at[my_z, my_y, my_x, my_core]
        elif stage == 1:
            count, source = rows_y, lambda: pieces.at[:, my_y, my_x, my_core]
        elif stage == 2:
            count, source = rows_x, lambda: pieces.at[:, :, my_x, my_core]
        else:
            count, source = cores, lambda: pieces.at[:, :, :, my_core]
        for hop in range(1, count):
            to = [my_z, my_y, my_x, my_core]
            to[stage] = lax.rem(to[stage] + hop, count)
            by = [my_z, my_y, my_x, my_core]
            by[stage] = lax.rem(by[stage] + count - hop, count)
            landed = pieces.at[(*(slice(None),) * stage, by[stage], *by[stage + 1 :])]
            if stage == 0:
                landed = pieces.at[by[0], my_y, my_x, my_core]
            pair = (layer, stage, hop)
            sems = dict(
                send_sem=piece_send_sems.at[pair],
                recv_sem=piece_recv_sems.at[pair],
                device_id=(at(*to),),
                device_id_type=MESH,
            )
            made.append(
                (
                    pltpu.make_async_remote_copy(src_ref=source(), dst_ref=source(), **sems),
                    pltpu.make_async_remote_copy(src_ref=landed, dst_ref=landed, **sems),
                )
            )
        return made

    def send_pieces(layer, stage):
        for out, _ in copies(layer, stage):
            out.start()

    def land_pieces(layer, stage):
        for out, landed in copies(layer, stage):
            out.wait_send()
            landed.wait_recv()

    def join_pieces(layer):
        pieces = (pieces_a, pieces_b)[layer]

        group = max(16 // share, 1)
        height = group * share

        def join(step, carry):
            for relation in range(relations + 1):
                rows = []
                for part in range(group):
                    device = step * group + part
                    z, rest = device // low, device % low
                    y, rest = rest // (rows_x * cores), rest % (rows_x * cores)
                    rows.append(
                        pieces[z, y, rest // cores, rest % cores, relation].astype(jnp.float32)
                    )
                first = pl.multiple_of(step * height, height)
                weight_ref[relation, pl.ds(first, height), :] = (
                    rows[0] if group == 1 else jnp.concatenate(rows, axis=0)
                ).astype(jnp.bfloat16)
            return carry

        lax.fori_loop(0, devices // group, join, 0)

    def peer_of(hop_z, hop_low, sign):
        z = lax.rem(my_z + planes + sign * hop_z, planes)
        rest = lax.rem(my_low + low + sign * hop_low, low)
        return z * low + rest

    def row_copy(layer, hop_z, hop_low, landing):
        came = (came_a, came_b)[layer]
        hop = hop_z * low + hop_low
        to = peer_of(hop_z, hop_low, 1)
        owner = peer_of(hop_z, hop_low, -1) if landing else me
        return pltpu.make_async_remote_copy(
            src_ref=sent.at[pl.ds(pl.multiple_of(to * slots, slots), slots)],
            dst_ref=came.at[pl.ds(pl.multiple_of(owner * slots, slots), slots)],
            send_sem=send_sems.at[layer, hop],
            recv_sem=recv_sems.at[layer, hop],
            device_id=(to,),
            device_id_type=MESH,
        )

    def plane_order():
        order = sorted(range(planes), key=lambda hop: -min(hop, planes - hop))
        return order[:1] + [0] * (planes > 1) + order[1:-1]

    def pick_planes(rows_ref, hops):
        starts = [
            pl.multiple_of(lax.rem(my_z + hop, planes) * plane_rows + part * 256, 256)
            for hop in hops
            for part in range(plane_rows // 256)
        ]
        columns = jnp.concatenate(
            [send_column_ref[pl.ds(first, 256), :] for first in starts], axis=0
        )
        rows = jnp.dot(
            one_hot(columns, 0, node_rows), rows_ref[...], preferred_element_type=jnp.float32
        ).astype(jnp.bfloat16)
        for part, first in enumerate(starts):
            sent[pl.ds(first, 256), :] = rows[part * 256 : (part + 1) * 256]

    def start_plane(layer, hop_z):
        def start(hop_low, carry):
            row_copy(layer, hop_z, hop_low, False).start()
            return carry

        lax.fori_loop(1 if hop_z == 0 else 0, low, start, 0)

    def land_plane(layer, hop_z):
        def land(hop_low, carry):
            row_copy(layer, hop_z, hop_low, False).wait_send()
            row_copy(layer, hop_z, hop_low, True).wait_recv()
            return carry

        lax.fori_loop(1 if hop_z == 0 else 0, low, land, 0)

    place_ids = lax.broadcasted_iota(jnp.int32, (places, edges), 0)

    def send_rows(layer, rows_ref):
        came = (came_a, came_b)[layer]
        came[pl.ds(pl.multiple_of(me * slots, slots), slots), :] = jnp.zeros(
            (slots, width), jnp.bfloat16
        )
        waiting = []
        hops = plane_order()
        for first in range(0, planes, 2):
            pick_planes(rows_ref, hops[first : first + 2])
            for hop in waiting:
                start_plane(layer, hop)
            waiting = hops[first : first + 2]
        return waiting

    def own_stage(rows_ref, spreading, between=None):
        group = group_of(node_rows, devices)

        def pick(step, first):
            part = pl.ds(first, group)
            hot = one_hot(column_ref[part].reshape(group * edges, 128), 0, node_rows)
            picked_ref[part] = (
                jnp.dot(hot, rows_ref[...], preferred_element_type=jnp.float32)
                .astype(jnp.bfloat16)
                .reshape(group, edges, width)
            )

        if spreading:
            group = min(group, 16)
            source_columns(0, group, True)
            for first in range(0, blocks, group):
                if first + group < blocks:
                    source_columns(first + group, group, False)
                pick(0, first)
                if between is not None and (first + group) * 4 == blocks * 3:
                    between()
        else:

            def body(step, carry):
                pick(step, step * group)
                return carry

            lax.fori_loop(0, blocks // group, body, 0)

    def plane_parts(layer, columns, hops):
        came = (came_a, came_b)[layer]
        total = None
        for hop_z in hops:
            z = lax.rem(my_z + planes - hop_z, planes)
            hot = one_hot(columns, node_rows + z * plane_rows, plane_rows)
            rows = came[pl.ds(pl.multiple_of(z * plane_rows, plane_rows), plane_rows), :]
            part = jnp.dot(hot, rows, preferred_element_type=jnp.float32)
            total = part if total is None else total + part
        return total.astype(jnp.bfloat16)

    def near_stage(layer, hops):
        group = group_of(plane_rows * len(hops), devices)

        def pick(step, carry):
            part = pl.ds(step * group, group)
            columns = column_ref[part].reshape(group * edges, 128)
            picked_ref[part] += plane_parts(layer, columns, hops).reshape(group, edges, width)
            return carry

        lax.fori_loop(0, blocks // group, pick, 0)

    def block_at(step):
        return jnp.clip(plan_smem[0, step], 0, blocks - 1)

    def last_of(window):
        return jnp.clip(plan_smem[2, window], 0, blocks)

    def hot_of(block):
        return (place_ids == slot_ref[block]).astype(jnp.float32).astype(jnp.bfloat16)

    def pool_stage(first, count):
        def pool(step, carry):
            total = pooled_ref[step * POOL]
            for part in range(POOL):
                block = block_at(step * POOL + part)
                sums = jnp.dot(
                    hot_of(block), picked_ref[block], preferred_element_type=jnp.float32
                )
                keep = plan_smem[1, step * POOL + part].astype(jnp.float32)
                total = total * keep + sums
                pooled_ref[step * POOL + part + 1] = total
            return carry

        steps = blocks // POOL
        lax.fori_loop(first * steps // 4, (first + count) * steps // 4, pool, 0)

    def degree_stage():
        ones = jnp.ones((edges, 128), jnp.bfloat16)

        def pool(step, carry):
            total = pooled_ref[step * COUNT, :, 0:128]
            for part in range(COUNT):
                block = block_at(step * COUNT + part)
                numbers = jnp.dot(hot_of(block), ones, preferred_element_type=jnp.float32)
                keep = plan_smem[1, step * COUNT + part].astype(jnp.float32)
                total = total * keep + numbers
                pooled_ref[step * COUNT + part + 1, :, 0:128] = total
            return carry

        lax.fori_loop(0, blocks // COUNT, pool, 0)

        def invert(step, carry):
            for part in range(4):
                window = step * 4 + part
                numbers = pooled_ref[last_of(window), :, 0:128]
                inverse_ref[window] = 1.0 / jnp.maximum(numbers, 1.0)
            return carry

        lax.fori_loop(0, windows // 4, invert, 0)

    def mean_stage():
        def average(step, carry):
            for window in [step * 4 + part for part in range(4)]:
                block = last_of(window)
                first = pl.multiple_of(window * WIN, WIN)
                for relation in range(relations):
                    part = slice(relation * WIN, (relation + 1) * WIN)
                    inverse = inverse_ref[window, part, :]
                    for lane in range(0, width, 128):
                        mean_ref[relation, pl.ds(first, WIN), lane : lane + 128] = (
                            pooled_ref[block, part, lane : lane + 128] * inverse
                        ).astype(jnp.bfloat16)
            return carry

        lax.fori_loop(0, windows // 4, average, 0)

    def dense_stage(rows_ref, bias_ref, result_ref, last):
        height = min(node_rows, 1024 if last else 512)

        def dense(chunk, carry):
            rows = pl.ds(pl.multiple_of(chunk * height, height), height)
            total = bias_ref[...] + jnp.dot(
                rows_ref[rows, :], weight_ref[relations], preferred_element_type=jnp.float32
            )
            for relation in range(relations):
                total = total + jnp.dot(
                    mean_ref[relation, rows, :],
                    weight_ref[relation],
                    preferred_element_type=jnp.float32,
                )
            if not last:
                total = jnp.maximum(total, 0.0)
            result_ref[rows, :] = total.astype(jnp.bfloat16)
            return carry

        lax.fori_loop(0, node_rows // height, dense, 0)

    def source_columns(start, count, mixed):
        if mixed:
            ones_wide = jnp.ones((2 * edges, 128), jnp.bfloat16)
        listed = source_ref[start : start + count, :]
        turned = turned_ref[...]
        small = listed % 128
        large = (listed - small).astype(jnp.float32)
        small = small.astype(jnp.float32)
        for row in range(count):
            if row % 2 or not mixed:
                column = jnp.broadcast_to(
                    turned[:, start + row : start + row + 1], (edges, 128)
                )
            else:
                diagonal = [
                    jnp.where(eye, one[row : row + 1, :], 0.0).astype(jnp.bfloat16)
                    for one in (large, small)
                ]
                column = jnp.dot(
                    jnp.concatenate(diagonal, axis=1),
                    ones_wide,
                    preferred_element_type=jnp.float32,
                )
            column_ref[start + row] = column.astype(jnp.int32)

    near = [0]
    far = [hop for hop in plane_order() if hop not in near]

    scope = jax.named_scope
    plan_copy = pltpu.make_async_copy(plan_ref, plan_smem, plan_sem)
    plan_copy.start()
    pooled_ref[0] = jnp.zeros(pooled_ref.shape[1:], jnp.float32)
    turned_ref[...] = jnp.transpose(source_ref[...].astype(jnp.float32))
    plan_copy.wait()
    with scope("degree"):
        degree_stage()
    with scope("greeted"):
        pl.semaphore_wait(barrier, devices - 1)
    send_pieces(0, 0)
    with scope("send_a"):
        waiting = send_rows(0, features_ref)
    with scope("compose_b"):
        compose(bases_b, self_b, coef_b, pieces_b)
    for hop in waiting:
        start_plane(0, hop)

    def forward():
        land_pieces(0, 0)
        send_pieces(0, 1)

    with scope("own_a"):
        own_stage(features_ref, True, forward)
    with scope("land_near_a"):
        for hop in near:
            land_plane(0, hop)
    with scope("near_a"):
        near_stage(0, near)
    with scope("piece_y"):
        land_pieces(0, 1)
    send_pieces(0, 2)
    send_pieces(1, 0)
    with scope("land_mid_a"):
        for hop in far[:1]:
            land_plane(0, hop)
    with scope("mid_a"):
        near_stage(0, far[:1])
    with scope("land_far_a"):
        for hop in far[1:]:
            land_plane(0, hop)
    with scope("far_a"):
        near_stage(0, far[1:])
    with scope("piece_x"):
        land_pieces(0, 2)
    send_pieces(0, 3)
    with scope("pool_a"):
        pool_stage(0, 4)
    with scope("piece_z_b"):
        land_pieces(1, 0)
    send_pieces(1, 1)
    with scope("mean_a"):
        mean_stage()
    with scope("piece_core"):
        land_pieces(0, 3)
    with scope("join_a"):
        join_pieces(0)
    with scope("dense_a"):
        dense_stage(features_ref, bias_a, out_ref, False)

    with scope("send_b"):
        waiting = send_rows(1, out_ref)
    for hop in waiting:
        start_plane(1, hop)
    with scope("piece_y_b"):
        land_pieces(1, 1)
    send_pieces(1, 2)
    with scope("own_b"):
        own_stage(out_ref, False)
    with scope("land_near_b"):
        for hop in near:
            land_plane(1, hop)
    with scope("near_b"):
        near_stage(1, near)
    with scope("land_far_b"):
        for hop in far:
            land_plane(1, hop)
    with scope("far_b"):
        near_stage(1, far)
    with scope("piece_x_b"):
        land_pieces(1, 2)
    send_pieces(1, 3)
    with scope("pool_b"):
        pool_stage(0, 4)
    with scope("mean_b"):
        mean_stage()
    with scope("piece_core_b"):
        land_pieces(1, 3)
    with scope("join_b"):
        join_pieces(1)
    with scope("dense_b"):
        dense_stage(out_ref, bias_b, out_ref, True)


def in_smem():
    return pl.BlockSpec(memory_space=pltpu.SMEM)


def in_vmem():
    return pl.BlockSpec(memory_space=pltpu.VMEM)


def shards(
    devices,
    features,
    edge_source,
    edge_relation,
    edge_target,
    block_count,
    send_list,
    bases_first,
    self_first,
    coef_first,
    bias_first,
    bases_second,
    self_second,
    coef_second,
    bias_second,
):
    node_rows, width = features.shape
    _, blocks, edges = edge_source.shape
    _, peers, slots = send_list.shape
    relations = coef_first.shape[0]
    share = self_first.shape[0]
    planes, rows_y, rows_x, cores = sides(devices)
    windows = node_rows // WIN
    places = WIN * relations
    came = peers * slots
    bf16, f32, i32 = jnp.bfloat16, jnp.float32, jnp.int32
    piece = (planes, rows_y, rows_x, cores, relations + 1, share, width)
    most = max(planes, rows_y, rows_x, cores)
    return pl.pallas_call(
        functools.partial(fused_kernel, devices),
        out_shape=pltpu.VMEM((node_rows, width), bf16),
        in_specs=[in_vmem()] * 4
        + [in_smem()]
        + [in_vmem()] * 5
        + [in_smem()] * 2
        + [in_vmem()] * 2,
        out_specs=in_vmem(),
        scratch_shapes=[
            pltpu.VMEM((blocks, edges, 128), i32),
            pltpu.VMEM((blocks, edges, width), bf16),
            pltpu.VMEM((blocks + 1, places, width), f32),
            pltpu.VMEM((windows, places, 128), f32),
            pltpu.VMEM((relations, node_rows, width), bf16),
            pltpu.VMEM((relations + 1, width, width), bf16),
            pltpu.VMEM(piece, bf16),
            pltpu.VMEM(piece, bf16),
            pltpu.VMEM((blocks, 1, edges), i32),
            pltpu.VMEM((came, 128), i32),
            pltpu.VMEM((came, width), bf16),
            pltpu.VMEM((came, width), bf16),
            pltpu.VMEM((came, width), bf16),
            pltpu.VMEM((8, 128), i32),
            pltpu.VMEM((edges, blocks), f32),
            pltpu.SMEM((8, 128), i32),
            pltpu.SemaphoreType.DMA,
            pltpu.SemaphoreType.DMA((2, peers)),
            pltpu.SemaphoreType.DMA((2, peers)),
            pltpu.SemaphoreType.DMA((2, 4, most)),
            pltpu.SemaphoreType.DMA((2, 4, most)),
        ],
        compiler_params=pltpu.CompilerParams(
            collective_id=0, has_side_effects=True, vmem_limit_bytes=VMEM_LIMIT
        ),
        name="rgcn",
    )(
        edge_source[0],
        edge_relation[0],
        edge_target[0],
        send_list[0],
        block_count[None],
        features,
        bases_first,
        self_first,
        bases_second,
        self_second,
        coef_first,
        coef_second,
        bias_first[None],
        bias_second[None],
    )


def solution(mesh):
    placed = (
        P("dom", None),
        P("dom", None, None),
        P("dom", None, None),
        P("dom", None, None),
        P("dom"),
        P("dom", None, None),
        P(None, "dom", None),
        P("dom", None),
        P(),
        P(),
        P(None, "dom", None),
        P("dom", None),
        P(),
        P(),
    )
    return jax.shard_map(
        functools.partial(shards, mesh.shape["dom"]),
        mesh=mesh,
        in_specs=placed,
        out_specs=P("dom", None),
        check_vma=False,
    )
```

```python
import functools
import math

import jax
import jax.numpy as jnp
from jax import lax
from jax.experimental import pallas as pl
from jax.experimental.pallas import tpu as pltpu
from jax.sharding import PartitionSpec as P

WIN = 16
POOL, COUNT = 32, 32
VMEM_LIMIT = 63 * 1024 * 1024
MESH = pl.DeviceIdType.MESH


def sides(devices):
    chips = devices // 2
    side = max(math.isqrt(chips // 4), 1)
    return chips // (side * side), side, side, 2


def group_of(depth, devices):
    group = 32
    while group * depth * devices > 1024 * 1024:
        group //= 2
    return group


def one_hot(columns, first, count):
    lanes = lax.broadcasted_iota(jnp.int32, columns.shape, 1)
    parts = [
        (columns == lanes + (first + part * 128)).astype(jnp.float32).astype(jnp.bfloat16)
        for part in range(count // 128)
    ]
    return jnp.concatenate(parts, axis=1)


def fused_kernel(
    devices,
    source_ref,
    relation_ref,
    target_ref,
    send_ref,
    count_ref,
    features_ref,
    bases_a,
    self_a,
    bases_b,
    self_b,
    coef_a,
    coef_b,
    bias_a,
    bias_b,
    out_ref,
    column_ref,
    picked_ref,
    pooled_ref,
    inverse_ref,
    mean_ref,
    weight_ref,
    pieces_a,
    pieces_b,
    slot_ref,
    send_column_ref,
    sent,
    came_a,
    came_b,
    plan_ref,
    turned_ref,
    plan_smem,
    plan_sem,
    send_sems,
    recv_sems,
    piece_send_sems,
    piece_recv_sems,
):
    me = lax.axis_index("dom")
    planes, rows_y, rows_x, cores = sides(devices)
    low = rows_y * rows_x * cores
    my_z, my_low = me // low, me % low
    my_y = my_low // (rows_x * cores)
    my_x = my_low // cores % rows_x
    my_core = my_low % cores
    node_rows, width = features_ref.shape
    blocks, edges = source_ref.shape
    peers, slots = send_ref.shape
    relations, bases = coef_a.shape
    share = self_a.shape[0]
    windows = node_rows // WIN
    places = WIN * relations
    plane_rows = low * slots

    def at(z, y, x, core):
        return ((z * rows_y + y) * rows_x + x) * cores + core

    barrier = pltpu.get_barrier_semaphore()

    def greet(hop, carry):
        peer = lax.rem(me + hop, devices)
        pl.semaphore_signal(barrier, inc=1, device_id=(peer,), device_id_type=MESH)
        return carry

    lax.fori_loop(1, devices, greet, 0)

    def compose(bases_ref, self_ref, coef_ref, pieces):
        sums = [jnp.zeros((share, width), jnp.float32) for _ in range(relations)]
        for basis in range(bases):
            matrix = bases_ref[basis].astype(jnp.float32)
            sums = [
                total + coef_ref[relation, basis] * matrix for relation, total in enumerate(sums)
            ]
        for relation, total in enumerate(sums):
            pieces[my_z, my_y, my_x, my_core, relation] = total.astype(jnp.bfloat16)
        pieces[my_z, my_y, my_x, my_core, relations] = self_ref[...]

    compose(bases_a, self_a, coef_a, pieces_a)

    lane_ids = lax.broadcasted_iota(jnp.int32, (edges, 128), 1)
    row_ids = lax.broadcasted_iota(jnp.int32, (edges, 128), 0)
    eye = row_ids == lane_ids
    eye_send = lax.broadcasted_iota(jnp.int32, (slots, slots), 0) == lax.broadcasted_iota(
        jnp.int32, (slots, slots), 1
    )

    def send_columns(group, carry):
        listed = send_ref[pl.ds(pl.multiple_of(group * 8, 8), 8), :]
        for row in range(8):
            spread = jnp.where(eye_send, listed[row : row + 1, :], 0).astype(jnp.float32)
            column = jnp.sum(spread, axis=1, keepdims=True)
            first = pl.multiple_of((group * 8 + row) * slots, slots)
            send_column_ref[pl.ds(first, slots), :] = jnp.broadcast_to(
                column, (slots, 128)
            ).astype(jnp.int32)
        return carry

    lax.fori_loop(0, peers // 8, send_columns, 0)

    def plan():
        window_c = jnp.broadcast_to(target_ref[:, 0:1] // WIN, (blocks, 128))
        window_r = jnp.sum(jnp.where(eye, window_c, 0), axis=0, keepdims=True)
        key_c = window_c * blocks + row_ids
        key_r = window_r * blocks + lane_ids[0:1]
        before = jnp.where(key_c < key_r, 1, 0)
        rank_r = jnp.sum(before, axis=0, keepdims=True)
        same = jnp.where(window_c == window_r, before, 0)
        follows_r = jnp.minimum(jnp.sum(same, axis=0, keepdims=True), 1)
        rank_c = jnp.transpose(jnp.broadcast_to(rank_r, (128, 128)))
        follows_c = jnp.transpose(jnp.broadcast_to(follows_r, (128, 128)))
        placed = rank_c == lane_ids
        order = jnp.sum(jnp.where(placed, row_ids, 0), axis=0, keepdims=True)
        keep = jnp.sum(jnp.where(placed, follows_c, 0), axis=0, keepdims=True)
        last = jnp.max(
            jnp.where(window_c == lane_ids, rank_c + 1, 0), axis=0, keepdims=True
        )
        plan_ref[...] = jnp.concatenate(
            [order, keep, last, jnp.zeros((5, 128), jnp.int32)], axis=0
        )

    plan()

    slot = relation_ref[...] * WIN + target_ref[...] % WIN
    slot_ref[...] = jnp.where(row_ids < count_ref[0, 0], slot, -1).reshape(blocks, 1, edges)

    def copies(layer, stage):
        pieces = (pieces_a, pieces_b)[layer]
        made = []
        if stage == 0:
            count, source = planes, lambda: pieces.at[my_z, my_y, my_x, my_core]
        elif stage == 1:
            count, source = rows_y, lambda: pieces.at[:, my_y, my_x, my_core]
        elif stage == 2:
            count, source = rows_x, lambda: pieces.at[:, :, my_x, my_core]
        else:
            count, source = cores, lambda: pieces.at[:, :, :, my_core]
        for hop in range(1, count):
            to = [my_z, my_y, my_x, my_core]
            to[stage] = lax.rem(to[stage] + hop, count)
            by = [my_z, my_y, my_x, my_core]
            by[stage] = lax.rem(by[stage] + count - hop, count)
            landed = pieces.at[(*(slice(None),) * stage, by[stage], *by[stage + 1 :])]
            if stage == 0:
                landed = pieces.at[by[0], my_y, my_x, my_core]
            pair = (layer, stage, hop)
            sems = dict(
                send_sem=piece_send_sems.at[pair],
                recv_sem=piece_recv_sems.at[pair],
                device_id=(at(*to),),
                device_id_type=MESH,
            )
            made.append(
                (
                    pltpu.make_async_remote_copy(src_ref=source(), dst_ref=source(), **sems),
                    pltpu.make_async_remote_copy(src_ref=landed, dst_ref=landed, **sems),
                )
            )
        return made

    def send_pieces(layer, stage):
        for out, _ in copies(layer, stage):
            out.start()

    def land_pieces(layer, stage):
        for out, landed in copies(layer, stage):
            out.wait_send()
            landed.wait_recv()

    def join_pieces(layer):
        pieces = (pieces_a, pieces_b)[layer]

        group = max(16 // share, 1)
        height = group * share

        def join(step, carry):
            for relation in range(relations + 1):
                rows = []
                for part in range(group):
                    device = step * group + part
                    z, rest = device // low, device % low
                    y, rest = rest // (rows_x * cores), rest % (rows_x * cores)
                    rows.append(
                        pieces[z, y, rest // cores, rest % cores, relation].astype(jnp.float32)
                    )
                first = pl.multiple_of(step * height, height)
                weight_ref[relation, pl.ds(first, height), :] = (
                    rows[0] if group == 1 else jnp.concatenate(rows, axis=0)
                ).astype(jnp.bfloat16)
            return carry

        lax.fori_loop(0, devices // group, join, 0)

    def peer_of(hop_z, hop_low, sign):
        z = lax.rem(my_z + planes + sign * hop_z, planes)
        rest = lax.rem(my_low + low + sign * hop_low, low)
        return z * low + rest

    def row_copy(layer, hop_z, hop_low, landing):
        came = (came_a, came_b)[layer]
        hop = hop_z * low + hop_low
        to = peer_of(hop_z, hop_low, 1)
        owner = peer_of(hop_z, hop_low, -1) if landing else me
        return pltpu.make_async_remote_copy(
            src_ref=sent.at[pl.ds(pl.multiple_of(to * slots, slots), slots)],
            dst_ref=came.at[pl.ds(pl.multiple_of(owner * slots, slots), slots)],
            send_sem=send_sems.at[layer, hop],
            recv_sem=recv_sems.at[layer, hop],
            device_id=(to,),
            device_id_type=MESH,
        )

    def plane_order():
        order = sorted(range(planes), key=lambda hop: -min(hop, planes - hop))
        return order[:1] + [0] * (planes > 1) + order[1:-1]

    def pick_planes(rows_ref, hops):
        starts = [
            pl.multiple_of(lax.rem(my_z + hop, planes) * plane_rows + part * 256, 256)
            for hop in hops
            for part in range(plane_rows // 256)
        ]
        columns = jnp.concatenate(
            [send_column_ref[pl.ds(first, 256), :] for first in starts], axis=0
        )
        rows = jnp.dot(
            one_hot(columns, 0, node_rows), rows_ref[...], preferred_element_type=jnp.float32
        ).astype(jnp.bfloat16)
        for part, first in enumerate(starts):
            sent[pl.ds(first, 256), :] = rows[part * 256 : (part + 1) * 256]

    def start_plane(layer, hop_z):
        def start(hop_low, carry):
            row_copy(layer, hop_z, hop_low, False).start()
            return carry

        lax.fori_loop(1 if hop_z == 0 else 0, low, start, 0)

    def land_plane(layer, hop_z):
        def land(hop_low, carry):
            row_copy(layer, hop_z, hop_low, False).wait_send()
            row_copy(layer, hop_z, hop_low, True).wait_recv()
            return carry

        lax.fori_loop(1 if hop_z == 0 else 0, low, land, 0)

    place_ids = lax.broadcasted_iota(jnp.int32, (places, edges), 0)

    def send_rows(layer, rows_ref):
        came = (came_a, came_b)[layer]
        came[pl.ds(pl.multiple_of(me * slots, slots), slots), :] = jnp.zeros(
            (slots, width), jnp.bfloat16
        )
        waiting = []
        hops = plane_order()
        for first in range(0, planes, 2):
            pick_planes(rows_ref, hops[first : first + 2])
            for hop in waiting:
                start_plane(layer, hop)
            waiting = hops[first : first + 2]
        return waiting

    def own_stage(rows_ref, spreading, between=None):
        group = group_of(node_rows, devices)

        def pick(step, first):
            part = pl.ds(first, group)
            hot = one_hot(column_ref[part].reshape(group * edges, 128), 0, node_rows)
            picked_ref[part] = (
                jnp.dot(hot, rows_ref[...], preferred_element_type=jnp.float32)
                .astype(jnp.bfloat16)
                .reshape(group, edges, width)
            )

        if spreading:
            group = min(group, 16)
            source_columns(0, group, True)
            for first in range(0, blocks, group):
                if first + group < blocks:
                    source_columns(first + group, group, False)
                pick(0, first)
                if between is not None and (first + group) * 4 == blocks * 3:
                    between()
        else:

            def body(step, carry):
                pick(step, step * group)
                return carry

            lax.fori_loop(0, blocks // group, body, 0)

    def plane_parts(layer, columns, hops):
        came = (came_a, came_b)[layer]
        total = None
        for hop_z in hops:
            z = lax.rem(my_z + planes - hop_z, planes)
            hot = one_hot(columns, node_rows + z * plane_rows, plane_rows)
            rows = came[pl.ds(pl.multiple_of(z * plane_rows, plane_rows), plane_rows), :]
            part = jnp.dot(hot, rows, preferred_element_type=jnp.float32)
            total = part if total is None else total + part
        return total.astype(jnp.bfloat16)

    def near_stage(layer, hops):
        group = group_of(plane_rows * len(hops), devices)

        def pick(step, carry):
            part = pl.ds(step * group, group)
            columns = column_ref[part].reshape(group * edges, 128)
            picked_ref[part] += plane_parts(layer, columns, hops).reshape(group, edges, width)
            return carry

        lax.fori_loop(0, blocks // group, pick, 0)

    def block_at(step):
        return jnp.clip(plan_smem[0, step], 0, blocks - 1)

    def last_of(window):
        return jnp.clip(plan_smem[2, window], 0, blocks)

    def hot_of(block):
        return (place_ids == slot_ref[block]).astype(jnp.float32).astype(jnp.bfloat16)

    def pool_stage(first, count):
        def pool(step, carry):
            total = pooled_ref[step * POOL]
            for part in range(POOL):
                block = block_at(step * POOL + part)
                sums = jnp.dot(
                    hot_of(block), picked_ref[block], preferred_element_type=jnp.float32
                )
                keep = plan_smem[1, step * POOL + part].astype(jnp.float32)
                total = total * keep + sums
                pooled_ref[step * POOL + part + 1] = total
            return carry

        steps = blocks // POOL
        lax.fori_loop(first * steps // 4, (first + count) * steps // 4, pool, 0)

    def degree_stage():
        ones = jnp.ones((edges, 128), jnp.bfloat16)

        def pool(step, carry):
            total = pooled_ref[step * COUNT, :, 0:128]
            for part in range(COUNT):
                block = block_at(step * COUNT + part)
                numbers = jnp.dot(hot_of(block), ones, preferred_element_type=jnp.float32)
                keep = plan_smem[1, step * COUNT + part].astype(jnp.float32)
                total = total * keep + numbers
                pooled_ref[step * COUNT + part + 1, :, 0:128] = total
            return carry

        lax.fori_loop(0, blocks // COUNT, pool, 0)

        def invert(step, carry):
            for part in range(4):
                window = step * 4 + part
                numbers = pooled_ref[last_of(window), :, 0:128]
                inverse_ref[window] = 1.0 / jnp.maximum(numbers, 1.0)
            return carry

        lax.fori_loop(0, windows // 4, invert, 0)

    def mean_stage():
        def average(step, carry):
            for window in [step * 4 + part for part in range(4)]:
                block = last_of(window)
                first = pl.multiple_of(window * WIN, WIN)
                for relation in range(relations):
                    part = slice(relation * WIN, (relation + 1) * WIN)
                    inverse = inverse_ref[window, part, :]
                    for lane in range(0, width, 128):
                        mean_ref[relation, pl.ds(first, WIN), lane : lane + 128] = (
                            pooled_ref[block, part, lane : lane + 128] * inverse
                        ).astype(jnp.bfloat16)
            return carry

        lax.fori_loop(0, windows // 4, average, 0)

    def dense_stage(rows_ref, bias_ref, result_ref, last):
        height = min(node_rows, 1024 if last else 512)

        def dense(chunk, carry):
            rows = pl.ds(pl.multiple_of(chunk * height, height), height)
            total = bias_ref[...] + jnp.dot(
                rows_ref[rows, :], weight_ref[relations], preferred_element_type=jnp.float32
            )
            for relation in range(relations):
                total = total + jnp.dot(
                    mean_ref[relation, rows, :],
                    weight_ref[relation],
                    preferred_element_type=jnp.float32,
                )
            if not last:
                total = jnp.maximum(total, 0.0)
            result_ref[rows, :] = total.astype(jnp.bfloat16)
            return carry

        lax.fori_loop(0, node_rows // height, dense, 0)

    def source_columns(start, count, mixed):
        if mixed:
            ones_wide = jnp.ones((2 * edges, 128), jnp.bfloat16)
        listed = source_ref[start : start + count, :]
        turned = turned_ref[...]
        small = listed % 128
        large = (listed - small).astype(jnp.float32)
        small = small.astype(jnp.float32)
        for row in range(count):
            if row % 2 or not mixed:
                column = jnp.broadcast_to(
                    turned[:, start + row : start + row + 1], (edges, 128)
                )
            else:
                diagonal = [
                    jnp.where(eye, one[row : row + 1, :], 0.0).astype(jnp.bfloat16)
                    for one in (large, small)
                ]
                column = jnp.dot(
                    jnp.concatenate(diagonal, axis=1),
                    ones_wide,
                    preferred_element_type=jnp.float32,
                )
            column_ref[start + row] = column.astype(jnp.int32)

    near = [0]
    far = [hop for hop in plane_order() if hop not in near]

    scope = jax.named_scope
    plan_copy = pltpu.make_async_copy(plan_ref, plan_smem, plan_sem)
    plan_copy.start()
    pooled_ref[0] = jnp.zeros(pooled_ref.shape[1:], jnp.float32)
    turned_ref[...] = jnp.transpose(source_ref[...].astype(jnp.float32))
    plan_copy.wait()
    with scope("degree"):
        degree_stage()
    with scope("greeted"):
        pl.semaphore_wait(barrier, devices - 1)
    send_pieces(0, 0)
    with scope("send_a"):
        waiting = send_rows(0, features_ref)
    with scope("compose_b"):
        compose(bases_b, self_b, coef_b, pieces_b)
    for hop in waiting:
        start_plane(0, hop)

    def forward():
        land_pieces(0, 0)
        send_pieces(0, 1)

    with scope("own_a"):
        own_stage(features_ref, True, forward)
    with scope("land_near_a"):
        for hop in near:
            land_plane(0, hop)
    with scope("near_a"):
        near_stage(0, near)
    with scope("piece_y"):
        land_pieces(0, 1)
    send_pieces(0, 2)
    send_pieces(1, 0)
    with scope("land_mid_a"):
        for hop in far[:1]:
            land_plane(0, hop)
    with scope("mid_a"):
        near_stage(0, far[:1])
    with scope("land_far_a"):
        for hop in far[1:]:
            land_plane(0, hop)
    with scope("far_a"):
        near_stage(0, far[1:])
    with scope("piece_x"):
        land_pieces(0, 2)
    send_pieces(0, 3)
    with scope("pool_a"):
        pool_stage(0, 4)
    with scope("piece_z_b"):
        land_pieces(1, 0)
    send_pieces(1, 1)
    with scope("mean_a"):
        mean_stage()
    with scope("piece_core"):
        land_pieces(0, 3)
    with scope("join_a"):
        join_pieces(0)
    with scope("dense_a"):
        dense_stage(features_ref, bias_a, out_ref, False)

    with scope("send_b"):
        waiting = send_rows(1, out_ref)
    for hop in waiting:
        start_plane(1, hop)
    with scope("own_b"):
        own_stage(out_ref, False)
    with scope("piece_y_b"):
        land_pieces(1, 1)
    send_pieces(1, 2)
    with scope("land_near_b"):
        for hop in near:
            land_plane(1, hop)
    with scope("near_b"):
        near_stage(1, near)
    with scope("land_far_b"):
        for hop in far:
            land_plane(1, hop)
    with scope("far_b"):
        near_stage(1, far)
    with scope("piece_x_b"):
        land_pieces(1, 2)
    send_pieces(1, 3)
    with scope("pool_b"):
        pool_stage(0, 4)
    with scope("mean_b"):
        mean_stage()
    with scope("piece_core_b"):
        land_pieces(1, 3)
    with scope("join_b"):
        join_pieces(1)
    with scope("dense_b"):
        dense_stage(out_ref, bias_b, out_ref, True)


def in_smem():
    return pl.BlockSpec(memory_space=pltpu.SMEM)


def in_vmem():
    return pl.BlockSpec(memory_space=pltpu.VMEM)


def shards(
    devices,
    features,
    edge_source,
    edge_relation,
    edge_target,
    block_count,
    send_list,
    bases_first,
    self_first,
    coef_first,
    bias_first,
    bases_second,
    self_second,
    coef_second,
    bias_second,
):
    node_rows, width = features.shape
    _, blocks, edges = edge_source.shape
    _, peers, slots = send_list.shape
    relations = coef_first.shape[0]
    share = self_first.shape[0]
    planes, rows_y, rows_x, cores = sides(devices)
    windows = node_rows // WIN
    places = WIN * relations
    came = peers * slots
    bf16, f32, i32 = jnp.bfloat16, jnp.float32, jnp.int32
    piece = (planes, rows_y, rows_x, cores, relations + 1, share, width)
    most = max(planes, rows_y, rows_x, cores)
    return pl.pallas_call(
        functools.partial(fused_kernel, devices),
        out_shape=pltpu.VMEM((node_rows, width), bf16),
        in_specs=[in_vmem()] * 4
        + [in_smem()]
        + [in_vmem()] * 5
        + [in_smem()] * 2
        + [in_vmem()] * 2,
        out_specs=in_vmem(),
        scratch_shapes=[
            pltpu.VMEM((blocks, edges, 128), i32),
            pltpu.VMEM((blocks, edges, width), bf16),
            pltpu.VMEM((blocks + 1, places, width), f32),
            pltpu.VMEM((windows, places, 128), f32),
            pltpu.VMEM((relations, node_rows, width), bf16),
            pltpu.VMEM((relations + 1, width, width), bf16),
            pltpu.VMEM(piece, bf16),
            pltpu.VMEM(piece, bf16),
            pltpu.VMEM((blocks, 1, edges), i32),
            pltpu.VMEM((came, 128), i32),
            pltpu.VMEM((came, width), bf16),
            pltpu.VMEM((came, width), bf16),
            pltpu.VMEM((came, width), bf16),
            pltpu.VMEM((8, 128), i32),
            pltpu.VMEM((edges, blocks), f32),
            pltpu.SMEM((8, 128), i32),
            pltpu.SemaphoreType.DMA,
            pltpu.SemaphoreType.DMA((2, peers)),
            pltpu.SemaphoreType.DMA((2, peers)),
            pltpu.SemaphoreType.DMA((2, 4, most)),
            pltpu.SemaphoreType.DMA((2, 4, most)),
        ],
        compiler_params=pltpu.CompilerParams(
            collective_id=0, has_side_effects=True, vmem_limit_bytes=VMEM_LIMIT
        ),
        name="rgcn",
    )(
        edge_source[0],
        edge_relation[0],
        edge_target[0],
        send_list[0],
        block_count[None],
        features,
        bases_first,
        self_first,
        bases_second,
        self_second,
        coef_first,
        coef_second,
        bias_first[None],
        bias_second[None],
    )


def solution(mesh):
    placed = (
        P("dom", None),
        P("dom", None, None),
        P("dom", None, None),
        P("dom", None, None),
        P("dom"),
        P("dom", None, None),
        P(None, "dom", None),
        P("dom", None),
        P(),
        P(),
        P(None, "dom", None),
        P("dom", None),
        P(),
        P(),
    )
    return jax.shard_map(
        functools.partial(shards, mesh.shape["dom"]),
        mesh=mesh,
        in_specs=placed,
        out_specs=P("dom", None),
        check_vma=False,
    )
```
